256 devices in a mesh: energy: 16 (over x, z_lo, core), kpt: 4 (over z_hi), layer: 4 (over y).
Axes of the slice: x: 4, y: 4, z: 8 (z_hi: 4, z_lo: 2; z = z_hi * 2 + z_lo), core: 2. Of those that a mesh axis runs over, the one named last changes fastest.
Arguments:
- energies: float32 [64], P(('energy', 'layer')), may hold values from -1.5 to 1.5
- momenta: float32 [4], P('kpt'), may hold values from 0 to 1
- energy_level: int32 [64], P(('energy', 'layer')), may hold values from 0 to 7
- momentum_level: int32 [4], P('kpt'), may hold values from 0 to 7
- energy_table: float32 [8], replicated, may hold values from 0.25 to 4
- momentum_table: float32 [8], replicated, may hold values from 0.25 to 4
- onsite: float32 [5, 256, 256], replicated, may hold values from -1 to 1, as said below
- broad: float32 [5, 256], replicated, may hold values from 1 to 4
- kdiag: float32 [5, 256], replicated, may hold values from 0.2 to 2
- fermi: float32 [5], replicated, may hold values from -1 to 1
- couplings: float32 [3, 256, 256], replicated, may hold values from -0.0624 to 0.0624
- bond_kind: int32 [4], replicated, may hold values from 0 to 2
Outputs:
- density: float32 [4, 2, 256, 256], P('layer', None, 'energy')
- current: float32 [4, 2, 256, 256], P('layer', None, 'energy')
The draws below stay inside these ranges and needn't reach their ends.
Inputs may be any that keep to these rules, and one draw needn't show every extreme that they name: Each block of onsite is symmetric.
All inputs are finite; a program needn't handle non-finite values.
Results may differ from the reference program's by a relative error of at most 0.0001.
Values sent between devices are 32-bit elements; how exact they have to be, the bound alone decides.
No kernel may reach another device: no remote copies, remote signals or barrier semaphores. Data moves between devices by JAX's collectives and lax.ppermute only.
A program may use at most 64 MiB of HBM per device.

```python
import math
import jax
import jax.numpy as jnp
from jax import lax

B = 256
NKIND = 3
LEVELS = 8
NL = 4
NLS = 5
NE = 64
NK = 4


def draw_onsite(key, part):
    first_key, second_key = jax.random.split(jax.random.fold_in(key, 17))
    raw = jax.random.normal(first_key, (NLS, B, B), jnp.float32) * 0.0069
    symmetric = (raw + jnp.swapaxes(raw, 1, 2)) * 0.7071
    levels = jax.random.uniform(second_key, (NLS, B), jnp.float32, -1.0, 1.0)
    identity = jnp.eye(B, dtype=jnp.float32)
    return symmetric * (1.0 - identity) + levels[:, :, None] * identity


def place_ends(result, stream_key, low, high):
    dims = result.shape
    spot = [jax.random.randint(jax.random.fold_in(stream_key, axis), (), 0, dims[axis]) for axis in range(len(dims))]
    result = result.at[tuple(spot)].set(low)
    longest = dims.index(max(dims))
    spot[longest] = (spot[longest] + 1) % dims[longest]
    return result.at[tuple(spot)].set(high)


def level_of(stream_key, dims, shards, low, high):
    def one(position, shards_of):
        steps = jax.random.uniform(jax.random.fold_in(jax.random.fold_in(stream_key, 6), position), (shards_of,), jnp.float32, low / len(shards), high / len(shards))
        return jnp.repeat(jnp.exp(steps), dims[position] // shards_of).reshape((-1,) + (1,) * (len(dims) - position - 1))

    loudness = one(*shards[0])
    for cut in shards[1:]:
        loudness = loudness * one(*cut)
    return loudness


def normal_values(rng, extent, width, reach, held_as=jnp.bfloat16):
    result = jax.random.normal(rng, extent, jnp.float32) * width
    return jnp.minimum(jnp.maximum(result, -reach), reach).astype(held_as)


def setup_inputs(seed: int = 0) -> dict:
    arg_keys = jax.random.split(jax.random.key(seed), 13)
    return {
        "energies": jnp.clip(jax.random.uniform(arg_keys[0], (NE,), jnp.float32, -1.5, 1.5) * level_of(arg_keys[0], (NE,), ((0, 64),), -0.4, 0.0), -1.5, 1.5),
        "momenta": jnp.clip(1.0 * jax.random.uniform(arg_keys[1], (NK,), jnp.float32) ** level_of(arg_keys[1], (NK,), ((0, 4),), -0.2, 0.2), 0.0, 1.0),
        "energy_level": place_ends(jax.random.randint(arg_keys[2], (NE,), 0, LEVELS), jax.random.fold_in(arg_keys[2], 1), 0, LEVELS - 1).astype(jnp.int32),
        "momentum_level": place_ends(jax.random.randint(arg_keys[3], (NK,), 0, LEVELS), jax.random.fold_in(arg_keys[3], 1), 0, LEVELS - 1).astype(jnp.int32),
        "energy_table": jnp.clip(jnp.exp(jax.random.uniform(arg_keys[4], (LEVELS,), jnp.float32, math.log(0.25), math.log(4.0))), 0.25, 4.0),
        "momentum_table": jnp.clip(jnp.exp(jax.random.uniform(arg_keys[5], (LEVELS,), jnp.float32, math.log(0.25), math.log(4.0))), 0.25, 4.0),
        "onsite": draw_onsite(jax.random.fold_in(arg_keys[12], 71), 0),
        "broad": jnp.clip(jnp.exp(jax.random.uniform(arg_keys[7], (NLS, B), jnp.float32, math.log(1.0), math.log(4.0))), 1.0, 4.0),
        "kdiag": jnp.clip(jnp.exp(jax.random.uniform(arg_keys[8], (NLS, B), jnp.float32, math.log(0.2), math.log(2.0))), 0.2, 2.0),
        "fermi": jnp.clip(jax.random.uniform(arg_keys[9], (NLS,), jnp.float32, -1.0, 1.0), -1.0, 1.0),
        "couplings": normal_values(arg_keys[10], (NKIND, B, B), 0.0104, 0.0624, jnp.float32),
        "bond_kind": place_ends(jax.random.randint(arg_keys[11], (NL,), 0, NKIND), jax.random.fold_in(arg_keys[11], 1), 0, NKIND - 1).astype(jnp.int32),
    }


exact_mode = lax.Precision.HIGHEST
thermal = 0.25


def real_dot(left, right):
    return jnp.matmul(left, right, precision=exact_mode)


def complex_dot(left, right):
    return (real_dot(left[0], right[0]) - real_dot(left[1], right[1]),
            real_dot(left[0], right[1]) + real_dot(left[1], right[0]))


def real_left(matrix, values):
    return (real_dot(matrix, values[0]), real_dot(matrix, values[1]))


def real_right(values, matrix):
    return (real_dot(values[0], matrix), real_dot(values[1], matrix))


def swap_last(array):
    return jnp.swapaxes(array, -1, -2)


def adjoint(values):
    return (swap_last(values[0]), -swap_last(values[1]))


def transpose_pair(values):
    return (swap_last(values[0]), swap_last(values[1]))


def diag_embed(vector):
    return vector[..., :, None] * jnp.eye(vector.shape[-1], dtype=vector.dtype)


def invert(matrix):
    diag_real = jnp.diagonal(matrix[0], axis1=-2, axis2=-1)
    diag_imag = jnp.diagonal(matrix[1], axis1=-2, axis2=-1)
    modulus = diag_real * diag_real + diag_imag * diag_imag
    start_real = diag_real / modulus
    start_imag = -diag_imag / modulus
    scaled_real = start_real[..., :, None] * matrix[0] - start_imag[..., :, None] * matrix[1]
    scaled_imag = start_real[..., :, None] * matrix[1] + start_imag[..., :, None] * matrix[0]
    both_real = scaled_real * start_real[..., None, :] - scaled_imag * start_imag[..., None, :]
    both_imag = scaled_real * start_imag[..., None, :] + scaled_imag * start_real[..., None, :]
    first = (2.0 * diag_embed(start_real) - both_real, 2.0 * diag_embed(start_imag) - both_imag)
    second = complex_dot(first, complex_dot(matrix, first))
    return (2.0 * first[0] - second[0], 2.0 * first[1] - second[1])


def forward_sweep(energy_pts, moment_pts, onsite, broad, kdiag, fermi, bonds):
    greens = []
    lessers = []
    for layer_at in range(onsite.shape[0]):
        shift = energy_pts[:, None] - moment_pts[:, None] * kdiag[layer_at][None, :]
        base_real = diag_embed(shift) - onsite[layer_at]
        base_imag = diag_embed(jnp.broadcast_to(0.5 * broad[layer_at], shift.shape))
        source = broad[layer_at][None, :] * jax.nn.sigmoid((fermi[layer_at] - energy_pts[:, None]) / thermal)
        if layer_at == 0:
            green = invert((base_real, base_imag))
            scaled = (green[0] * source[:, None, :], green[1] * source[:, None, :])
            lesser = complex_dot(scaled, adjoint(green))
        else:
            bond = bonds[layer_at - 1]
            self_part = real_right(real_left(swap_last(bond), greens[-1]), bond)
            green = invert((base_real - self_part[0], base_imag - self_part[1]))
            inflow = real_right(real_left(swap_last(bond), lessers[-1]), bond)
            lesser = complex_dot(complex_dot(green, (inflow[0] + diag_embed(source), inflow[1])), adjoint(green))
        greens.append(green)
        lessers.append(lesser)
    return greens, lessers


def backward_step(green, lesser, bond, right_green, right_lesser):
    hopping = real_right(green, bond)
    carried = complex_dot(hopping, right_green)
    spread_green = complex_dot(carried, transpose_pair(hopping))
    new_green = (green[0] + spread_green[0], green[1] + spread_green[1])
    hop_lesser = complex_dot(hopping, right_lesser)
    through = complex_dot(right_green, real_left(swap_last(bond), lesser))
    cross = complex_dot(hopping, through)
    cross_adj = adjoint(cross)
    spread = complex_dot(hop_lesser, adjoint(hopping))
    new_lesser = (lesser[0] + spread[0] + cross[0] + cross_adj[0],
                  lesser[1] + spread[1] + cross[1] + cross_adj[1])
    through_adj = adjoint(through)
    current = (hop_lesser[0] + through_adj[0], hop_lesser[1] + through_adj[1])
    return new_green, new_lesser, current


def weighted_sum(weights, values):
    return jnp.stack([jnp.tensordot(weights, values[0], axes=1, precision=exact_mode),
                      jnp.tensordot(weights, values[1], axes=1, precision=exact_mode)])


def pick_rows(levels, table):
    count = table.shape[0]
    onehot = (levels[:, None] == jnp.arange(count, dtype=jnp.int32)[None, :]).astype(table.dtype)
    return jnp.sum(onehot * table[None, :], axis=1)


def reference(energies, momenta, energy_level, momentum_level, energy_table, momentum_table, onsite, broad, kdiag, fermi, couplings, bond_kind):
    kinds = couplings.shape[0]
    choose = (bond_kind[:, None] == jnp.arange(kinds, dtype=jnp.int32)[None, :]).astype(couplings.dtype)
    bonds = jnp.tensordot(choose, couplings, axes=1, precision=exact_mode)
    energy_weight = pick_rows(energy_level, energy_table)
    moment_weight = pick_rows(momentum_level, momentum_table)
    scale = 1.0 / (NE * NK)
    layers = onsite.shape[0] - 1

    def accumulate(carry, index):
        energy_pts = jnp.broadcast_to(energies[index], momenta.shape)
        weights = energy_weight[index] * moment_weight * scale
        greens, lessers = forward_sweep(energy_pts, momenta, onsite, broad, kdiag, fermi, bonds)
        right_green = greens[layers]
        right_lesser = lessers[layers]
        density_rows = [None] * layers
        current_rows = [None] * layers
        for layer_at in range(layers - 1, -1, -1):
            right_green, right_lesser, current = backward_step(greens[layer_at], lessers[layer_at], bonds[layer_at], right_green, right_lesser)
            density_rows[layer_at] = weighted_sum(weights, right_lesser)
            current_rows[layer_at] = weighted_sum(weights, current)
        return (carry[0] + jnp.stack(density_rows), carry[1] + jnp.stack(current_rows)), None

    zeros = jnp.zeros((layers, 2, onsite.shape[1], onsite.shape[1]), energies.dtype)
    totals = lax.scan(accumulate, (zeros, zeros), jnp.arange(NE, dtype=jnp.int32))[0]
    return totals[0], totals[1]
```

```python
import jax
import jax.numpy as jnp
from jax import lax
from jax.experimental import pallas as pl
from jax.experimental.pallas import tpu as pltpu
from jax.sharding import PartitionSpec as P

N = 256
ROWS = 256
CH = 32
f32 = jnp.float32
bf16 = jnp.bfloat16


def step_of(at, swap):
    first, second = at >> 1, at & 1
    plain = first ^ (3 * second)
    return plain ^ (swap * 2 * (first ^ second))


def slot_of(delta, swap):
    second = delta >> 1
    first = (delta & 1) ^ second
    plain = first * 2 + second
    return plain ^ (swap * 3 * (first ^ second))


def place():
    energy = lax.axis_index("energy")
    core = energy & 1
    return energy >> 2, lax.axis_index("layer"), (energy >> 1) & 1, core, core


def charge_kernel(pe, pk, elev, mlev, etab, mtab, fermi, kind, onsite, broad, kdiag, coup, keep, send, S, X, done):
    where_x, where_y, my_z, my_core, swap = place()
    slots = {}
    def slot(name):
        if name not in slots:
            slots[name] = len(slots)
            assert len(slots) <= S.shape[0], len(slots)
        return slots[name]
    fl = {}
    def fslot(name):
        if name not in fl:
            fl[name] = len(fl)
            assert len(fl) <= X.shape[0], len(fl)
        return fl[name]
    def put(name, r, x):
        i = slot(name)
        hi = x.astype(bf16)
        S[i, 0, r, :] = hi
        S[i, 1, r, :] = (x - hi.astype(f32)).astype(bf16)
    def mm(a, b, r, tb=False):
        a = slot(a); b = slot(b)
        dn = (((1,), (1 if tb else 0,)), ((), ()))
        d = lambda x, y: lax.dot_general(x, y, dn, preferred_element_type=f32)
        ah = S[a, 0, r, :]
        return d(ah, S[b, 0]) + d(ah, S[b, 1]) + d(S[a, 1, r, :], S[b, 0])
    def blocks(fn, post):
        for r0 in range(0, N, ROWS):
            vals = fn(slice(r0, r0 + ROWS))
            for c0 in range(0, ROWS, CH):
                post(slice(r0 + c0, r0 + c0 + CH), *[v[c0:c0 + CH] for v in vals])
    def pieces(post):
        for c0 in range(0, N, CH):
            post(slice(c0, c0 + CH))
    cols = lambda: lax.broadcasted_iota(jnp.int32, (CH, N), 1)
    def eye(r):
        return (lax.broadcasted_iota(jnp.int32, (CH, N), 0) + r.start) == cols()
    def result(comp, r, x):
        for c0 in range(0, r.stop - r.start, 16):
            done[comp, (r.start + c0) // 16] = x[c0:c0 + 16]
    def hand_out(layer):
        for core_at, to in ((0, keep), (1, send)):
            turn = swap ^ core_at
            y_at = slot_of(layer ^ where_y, turn)
            for x_at in range(4):
                x_from = where_x ^ step_of(x_at, turn)
                for z_at in range(2):
                    chunk = x_from * 4 + (my_z ^ z_at) * 2 + (my_core ^ core_at)
                    for comp in range(2):
                        to[0, x_at * 8 + y_at * 2 + z_at, comp] = done[comp, chunk]
                        to[1, y_at * 8 + x_at * 2 + z_at, comp] = done[2 + comp, chunk]
    e = pe[0]; k = pk[0]
    weight = etab[elev[0]] * mtab[mlev[0]] * (1.0 / 256)
    for i in range(4):
        def one(r, i=i):
            put(f"V{i}", r, coup[kind[i], r, :])
        pieces(one)
        vt = coup[kind[i]].T
        pieces(lambda r: put(f"Vt{i}", r, vt[r]))

    for i in range(5):
        shift = e - k * kdiag[i:i + 1, :]
        gamma = broad[i:i + 1, :] * jax.nn.sigmoid(jnp.full((1, N), (fermi[i] - e) / 0.25, f32))
        half = 0.5 * broad[i:i + 1, :]
        mr = fslot("mr"); mi = fslot("mi")
        if i:
            blocks(lambda r: (mm(f"Vt{i-1}", f"u{i-1}", r), mm(f"Vt{i-1}", f"v{i-1}", r)), lambda r, s, d: (
                X.__setitem__((mr, r), onsite[i, r, :] + 0.5 * (s + d)), X.__setitem__((mi, r), 0.5 * (s - d))))
            blocks(lambda r: (mm(f"Vt{i-1}", f"U{i-1}", r),), lambda r, y: put("C", r, y + jnp.where(eye(r), gamma, 0.0)))
            getr = lambda r: X[mr, r, :]
            geti = lambda r: X[mi, r, :]
        else:
            getr = lambda r: onsite[0, r, :]
        dr = jnp.zeros((1, N), f32); di = jnp.zeros((1, N), f32)
        for c0 in range(0, N, CH):
            r = slice(c0, c0 + CH)
            dr = dr + jnp.sum(jnp.where(eye(r), getr(r), 0.0), axis=0, keepdims=True)
            if i:
                di = di + jnp.sum(jnp.where(eye(r), geti(r), 0.0), axis=0, keepdims=True)
        dr = shift - dr
        di = half - di
        mod = dr * dr + di * di
        zr = dr / mod; zi = -di / mod
        size = jnp.sqrt(zr * zr + zi * zi)
        t = jnp.sqrt(0.5 * (size + jnp.abs(zr)))
        o = 0.5 * zi / t
        pos = zr >= 0.0
        rr = jnp.where(pos, t, jnp.abs(o))
        ri = jnp.where(pos, o, jnp.where(zi < 0.0, -t, t))
        crs = []; cis = []
        def outer(r):
            m = eye(r)
            cr = jnp.sum(jnp.where(m, rr, 0.0), axis=1, keepdims=True)
            ci = jnp.sum(jnp.where(m, ri, 0.0), axis=1, keepdims=True)
            return cr * rr - ci * ri, cr * ri + ci * rr
        orr = fslot("or"); oi = fslot("oi"); hr_ = fslot("hr"); hi_ = fslot("hi")
        def make_h(r):
            a, b = outer(r)
            X[orr, r] = a; X[oi, r] = b
            m = eye(r)
            er = jnp.where(m, 0.0, -getr(r))
            if i:
                ei = jnp.where(m, 0.0, -geti(r))
                hr = er * a - ei * b; hi = er * b + ei * a
            else:
                hr = er * a; hi = er * b
            X[hr_, r] = hr; X[hi_, r] = hi
            put("Hr", r, hr); put("Hi", r, hi); put("Hs", r, hr + hi)
        pieces(make_h)
        sr_ = fslot("sr"); si_ = fslot("si")
        def sq(r, a, b, c):
            sr = a - b
            X[sr_, r] = sr; X[si_, r] = c - a - b
            put("Sr", r, sr); put("Sa", r, c - 2.0 * a); put("Sb", r, c - 2.0 * b)
        blocks(lambda r: (mm("Hr", "Hr", r), mm("Hi", "Hi", r), mm("Hs", "Hs", r)), sq)
        def fin(r, k1, k2, k3):
            kr = X[sr_, r] - X[hr_, r] - (k1 - k3) + jnp.where(eye(r), 1.0, 0.0)
            ki = X[si_, r] - X[hi_, r] - (k1 + k2)
            a = X[orr, r]; b = X[oi, r]
            gr = kr * a - ki * b; gi = kr * b + ki * a
            gs = gr + gi; gd = gr - gi
            put(f"gs", r, gs); put(f"gd", r, gd)
            if 0 < i < 4:
                X[fslot(f"gs{i}"), r] = gs; X[fslot(f"gd{i}"), r] = gd
            if i == 4:
                put("Gs", r, gs); put("Gd", r, gd)
            if i == 0:
                put("p", r, gr * gamma); put("q", r, gi * gamma)
        blocks(lambda r: (mm("Hs", "Sr", r), mm("Hr", "Sa", r), mm("Hi", "Sb", r)), fin)
        if i < 4:
            blocks(lambda r: (mm("gs", f"V{i}", r), mm("gd", f"V{i}", r)), lambda r, u, v: (put(f"u{i}", r, u), put(f"v{i}", r, v)))
        if i:
            blocks(lambda r: (mm("gd", "C", r) + mm("gs", "C", r, True),), lambda r, p: put("p", r, 0.5 * p))
            blocks(lambda r: (mm("gs", "C", r), mm("gd", "C", r, True),), lambda r, a, b: put("q", r, 0.5 * (a - b)))
        w_ = fslot(f"w{i}")
        if i < 4:
            def keep_w(r, w):
                X[w_, r] = w
                put("W", r, w)
            blocks(lambda r: (mm("p", "gd", r) + mm("q", "gs", r),), keep_w)
            wt = X[w_].T
            pieces(lambda r: put("Wt", r, wt[r]))
            blocks(lambda r: (mm("W", f"V{i}", r), mm("Wt", f"V{i}", r)), lambda r, a, b: (put(f"U{i}", r, a), put(f"T{i}", r, b)))
        else:
            blocks(lambda r: (mm("p", "gd", r) + mm("q", "gs", r),), lambda r, w: put("W", r, w))

    for i in (3, 2, 1, 0):
        u = f"u{i}"; v = f"v{i}"; U = f"U{i}"; T = f"T{i}"
        def bond_r(r, a, b):
            result(2, r, (0.5 * weight) * (a + b))
            put("Yr", r, 0.25 * a + 0.5 * b)
        def bond_i(r, a, b, c, d):
            a = a - b; c = c - d
            result(3, r, (0.5 * weight) * (a + c))
            put("Yi", r, 0.25 * a + 0.5 * c)
        blocks(lambda r: (mm(v, "W", r) + mm(u, "W", r, True), mm(U, "Gs", r) + mm(T, "Gd", r)), bond_r)
        blocks(lambda r: (mm(u, "W", r), mm(v, "W", r, True), mm(U, "Gd", r), mm(T, "Gs", r)), bond_i)
        n_ = fslot("mr")
        def new_w(r, a, b):
            w = X[fslot(f"w{i}"), r] + a - b
            X[n_, r] = w
            if i:
                put("Wn", r, w)
        blocks(lambda r: (mm("Yr", v, r, True) + mm("Yi", u, r, True) + mm(u, "Yr", r, True), mm(v, "Yi", r, True)), new_w)
        wt = X[n_].T
        def dens(r):
            a = X[n_, r]; b = wt[r]
            result(0, r, (0.5 * weight) * (a + b))
            result(1, r, (0.5 * weight) * (a - b))
        pieces(dens)
        hand_out(i)
        slots["W"], slots["Wn"] = slots.get("Wn", 0), slots["W"]
        if i:
            blocks(lambda r: (mm(u, "Gd", r) + mm(v, "Gs", r),), lambda r, a: put("Qr", r, 0.5 * a))
            blocks(lambda r: (mm(u, "Gs", r), mm(v, "Gd", r)), lambda r, a, b: put("Qi", r, 0.5 * (a - b)))
            blocks(lambda r: (mm("Qr", u, r, True) + mm("Qi", v, r, True),), lambda r, a: put("Gs", r, X[fslot(f"gs{i}"), r] + a))
            blocks(lambda r: (mm("Qr", v, r, True), mm("Qi", u, r, True)), lambda r, a, b: put("Gd", r, X[fslot(f"gd{i}"), r] + a - b))


def charge(*arrays):
    smem = pl.BlockSpec(memory_space=pltpu.SMEM)
    vmem = pl.BlockSpec(memory_space=pltpu.VMEM)
    shape = jax.ShapeDtypeStruct((2, 32, 2, 16, N), f32)
    return pl.pallas_call(
        charge_kernel,
        out_shape=(shape, shape),
        in_specs=[smem] * 8 + [vmem] * 4,
        out_specs=(vmem, vmem),
        scratch_shapes=[
            pltpu.VMEM((48, 2, N, N), bf16),
            pltpu.VMEM((24, N, N), f32),
            pltpu.VMEM((4, 16, 16, N), f32),
        ],
        compiler_params=pltpu.CompilerParams(vmem_limit_bytes=56 * 1024 * 1024),
    )(*arrays)


def swapped(x, axes, partner):
    sizes = [lax.axis_size(a) for a in axes]
    count = 1
    for s in sizes:
        count *= s
    return lax.ppermute(x, axes, [(i, partner(i)) for i in range(count)])


def over_core(x):
    return swapped(x, ("energy",), lambda i: i ^ 1)


def over_x(x, turn):
    return swapped(x, ("energy",), lambda i: i ^ (12 if (i & 1) ^ turn else 4))


def over_y(x, turn):
    return swapped(x, ("energy", "layer"), lambda i: i ^ (3 if ((i >> 2) & 1) ^ turn else 1))


def over_z(x):
    return swapped(x, ("energy",), lambda i: i ^ 2)


def per_device(energies, momenta, energy_level, momentum_level, energy_table, momentum_table, onsite, broad, kdiag, fermi, couplings, bond_kind):
    keep, send = charge(energies, momenta, energy_level, momentum_level, energy_table, momentum_table, fermi, bond_kind, onsite, broad, kdiag, couplings)
    got = over_core(send)
    parts = [(keep[0], got[0]), (keep[1], got[1])]
    count = 32
    for across in ((over_x, over_y), (over_y, over_x)):
        for turn in range(2):
            count //= 2
            away = [mine[count:] + other[count:] for mine, other in parts]
            got = [across[g](away[g], turn) for g in range(2)]
            parts = [(mine[:count] + other[:count], got[g]) for g, (mine, other) in enumerate(parts)]
    away = jnp.stack([mine[1] + other[1] for mine, other in parts])
    got = over_z(away)
    mine = jnp.stack([mine[0] + other[0] for mine, other in parts]) + got
    near, far, last = (swapped(mine, ("kpt",), lambda i, s=s: i ^ s) for s in (1, 2, 3))
    total = (mine + near) + (far + last)
    return total[0][None], total[1][None]


def solution(mesh):
    return jax.shard_map(
        per_device,
        mesh=mesh,
        in_specs=(P(("energy", "layer")), P("kpt"), P(("energy", "layer")), P("kpt"), P(), P(), P(), P(), P(), P(), P(), P()),
        out_specs=(P("layer", None, "energy", None), P("layer", None, "energy", None)),
        check_vma=False,
    )
```

```python
import jax
import jax.numpy as jnp
from jax import lax
from jax.experimental import pallas as pl
from jax.experimental.pallas import tpu as pltpu
from jax.sharding import PartitionSpec as P

N = 256
CH = 32
f32 = jnp.float32
bf16 = jnp.bfloat16
KEPT = ("u0", "v0", "U0", "T0", "u1", "v1", "U1", "T1", "W2", "Gs2", "Gd2", "Gs1", "Gd1")
KEPT_FULL = ("w0", "w1", "weight")


def step_of(at, swap):
    first, second = at >> 1, at & 1
    plain = first ^ (3 * second)
    return plain ^ (swap * 2 * (first ^ second))


class Parts:
    def __init__(self, pairs, full, kept_pairs=None, kept_full=None):
        self.pairs, self.full = pairs, full
        self.at, self.full_at = {}, {}
        self.kept = {} if kept_pairs is None else {n: (kept_pairs, i) for i, n in enumerate(KEPT)}
        self.kept_full = {} if kept_full is None else {n: (kept_full, i) for i, n in enumerate(KEPT_FULL)}

    def pair(self, name):
        if name in self.kept:
            return self.kept[name]
        i = self.at.setdefault(name, len(self.at))
        assert i < self.pairs.shape[0]
        return self.pairs, i

    def whole(self, name):
        if name in self.kept_full:
            return self.kept_full[name]
        i = self.full_at.setdefault(name, len(self.full_at))
        assert i < self.full.shape[0]
        return self.full, i

    def put(self, name, r, x):
        ref, i = self.pair(name)
        high = x.astype(bf16)
        ref[i, 0, r, :] = high
        ref[i, 1, r, :] = (x - high.astype(f32)).astype(bf16)

    def store(self, name, r, x):
        ref, i = self.whole(name)
        ref[i, r, :] = x

    def load(self, name, r):
        ref, i = self.whole(name)
        return ref[i, r, :]

    def turned(self, name):
        ref, i = self.whole(name)
        return ref[i].T

    def mm(self, left, right, turn=False):
        a, i = self.pair(left)
        b, j = self.pair(right)
        contract = (((1,), (1 if turn else 0,)), ((), ()))

        def dot(x, y):
            return lax.dot_general(x, y, contract, preferred_element_type=f32)

        high = a[i, 0]
        return dot(high, b[j, 0]) + dot(high, b[j, 1]) + dot(a[i, 1], b[j, 0])


def pieces(post, *values):
    for c0 in range(0, N, CH):
        r = slice(c0, c0 + CH)
        post(r, *[v[r] for v in values])


def eye(r):
    rows = lax.broadcasted_iota(jnp.int32, (CH, N), 0) + r.start
    return rows == lax.broadcasted_iota(jnp.int32, (CH, N), 1)


def hand_out(layer, done, keep, send):
    energy = lax.axis_index("energy")
    core = energy & 1
    my_x, my_z = energy >> 2, (energy >> 1) & 1
    where_y = lax.axis_index("layer")
    y_at = (layer ^ (layer >> 1) ^ where_y ^ (where_y >> 1)) & 1
    for core_at, to in ((0, keep), (1, send)):
        for x_at in range(4):
            x_from = my_x ^ step_of(x_at, core ^ core_at)
            for z_at in range(2):
                chunk = x_from * 4 + (my_z ^ z_at) * 2 + (core ^ core_at)
                for comp in range(4):
                    to[x_at * 4 + y_at * 2 + z_at, comp] = done[comp, chunk]


def back_products(m, i, weight, done):
    u, v, U, T = f"u{i}", f"v{i}", f"U{i}", f"T{i}"
    W, Gs, Gd = f"W{i + 1}", f"Gs{i + 1}", f"Gd{i + 1}"

    def result(comp, r, x):
        for c0 in range(0, CH, 16):
            done[comp, (r.start + c0) // 16] = x[c0 : c0 + 16]

    def bond_re(r, a, b):
        result(2, r, weight * (0.5 * (a + b)))
        m.put("Yr", r, 0.25 * a + 0.5 * b)

    def bond_im(r, a, b, c, d):
        a, c = a - b, c - d
        result(3, r, weight * (0.5 * (a + c)))
        m.put("Yi", r, 0.25 * a + 0.5 * c)

    def bond():
        pieces(bond_re, m.mm(v, W) + m.mm(u, W, True), m.mm(U, Gs) + m.mm(T, Gd))
        pieces(bond_im, m.mm(u, W), m.mm(v, W, True), m.mm(U, Gd), m.mm(T, Gs))

    def new_w(r, a, b):
        w = m.load(f"w{i}", r) + a - b
        m.store("Wfull", r, w)
        if i:
            m.put(f"W{i}", r, w)

    def density():
        pieces(new_w, m.mm("Yr", v, True) + m.mm("Yi", u, True) + m.mm(u, "Yr", True), m.mm(v, "Yi", True))

    def dens(r, turned):
        a = m.load("Wfull", r)
        result(0, r, weight * (0.5 * (a + turned)))
        result(1, r, weight * (0.5 * (a - turned)))

    def report():
        pieces(dens, m.turned("Wfull"))

    def carry():
        pieces(lambda r, a: m.put("Qr", r, 0.5 * a), m.mm(u, Gd) + m.mm(v, Gs))
        pieces(lambda r, a, b: m.put("Qi", r, 0.5 * (a - b)), m.mm(u, Gs), m.mm(v, Gd))

    def spread():
        pieces(lambda r, a: m.put(f"Gs{i}", r, m.load(f"gs{i}", r) + a), m.mm("Qr", u, True) + m.mm("Qi", v, True))
        pieces(lambda r, a, b: m.put(f"Gd{i}", r, m.load(f"gd{i}", r) + a - b), m.mm("Qr", v, True), m.mm("Qi", u, True))

    return bond, density, report, carry, spread


def forward_kernel(*refs):
    arrays, (keep, send, kept_pairs, kept_full, pairs, full, done), local, sems = refs[4:12], refs[12:19], refs[19:27], refs[27]
    pe, pk, elev, mlev = refs[:4]
    etab, mtab, fermi, kind, broad, kdiag, onsite, coup = local
    small = [pltpu.make_async_copy(arrays[n], local[n], sems.at[n]) for n in range(6)]
    blocks = [pltpu.make_async_copy(arrays[6].at[n], onsite.at[n], sems.at[6 + n]) for n in range(5)]
    hops = pltpu.make_async_copy(arrays[7], coup, sems.at[11])
    for copy in small + blocks[:1] + [hops] + blocks[1:]:
        copy.start()
    m = Parts(pairs, full, kept_pairs, kept_full)
    for copy in small:
        copy.wait()
    e = pe[0]
    k = pk[0]
    weight = jnp.full((1, N), etab[elev[0]] * mtab[mlev[0]] * (1.0 / 256), f32)
    kept_full[KEPT_FULL.index("weight"), 0:8, :] = jnp.broadcast_to(weight, (8, N))

    def source(i):
        return broad[i : i + 1, :] * jax.nn.sigmoid(jnp.full((1, N), (fermi[i] - e) / 0.25, f32))

    def real_part(i, r):
        return m.load("mr", r) if i else onsite[0, r, :]

    def own_energy(i):
        def post(r, s, d):
            m.store("mr", r, onsite[i, r, :] + 0.5 * (s + d))
            m.store("mi", r, 0.5 * (s - d))

        blocks[i].wait()
        pieces(post, m.mm(f"Vt{i - 1}", f"u{i - 1}"), m.mm(f"Vt{i - 1}", f"v{i - 1}"))

    def scale(i):
        dr = jnp.zeros((1, N), f32)
        di = jnp.zeros((1, N), f32)
        for c0 in range(0, N, CH):
            r = slice(c0, c0 + CH)
            dr = dr + jnp.sum(jnp.where(eye(r), real_part(i, r), 0.0), axis=0, keepdims=True)
            if i:
                di = di + jnp.sum(jnp.where(eye(r), m.load("mi", r), 0.0), axis=0, keepdims=True)
        dr = e - k * kdiag[i : i + 1, :] - dr
        di = 0.5 * broad[i : i + 1, :] - di
        modulus = dr * dr + di * di
        zr = dr / modulus
        zi = -di / modulus
        size = jnp.sqrt(zr * zr + zi * zi)
        large = jnp.sqrt(0.5 * (size + jnp.abs(zr)))
        other = 0.5 * zi / large
        rr = jnp.where(zr >= 0.0, large, jnp.abs(other))
        ri = jnp.where(zr >= 0.0, other, jnp.where(zi < 0.0, -large, large))

        def post(r):
            mask = eye(r)
            cr = jnp.sum(jnp.where(mask, rr, 0.0), axis=1, keepdims=True)
            ci = jnp.sum(jnp.where(mask, ri, 0.0), axis=1, keepdims=True)
            a = cr * rr - ci * ri
            b = cr * ri + ci * rr
            m.store("or", r, a)
            m.store("oi", r, b)
            er = jnp.where(mask, 0.0, -real_part(i, r))
            if i:
                ei = jnp.where(mask, 0.0, -m.load("mi", r))
                hr, hi = er * a - ei * b, er * b + ei * a
            else:
                hr, hi = er * a, er * b
            m.store("hr", r, hr)
            m.store("hi", r, hi)
            m.put("Hr", r, hr)
            m.put("Hi", r, hi)
            m.put("Hs", r, hr + hi)

        pieces(post)

    def square(i):
        def post(r, a, b, c):
            m.store("sr", r, a - b)
            m.store("si", r, c - a - b)
            m.put("Sr", r, a - b)
            m.put("Sa", r, c - 2.0 * a)
            m.put("Sb", r, c - 2.0 * b)

        pieces(post, m.mm("Hr", "Hr"), m.mm("Hi", "Hi"), m.mm("Hs", "Hs"))

    def green(i):
        def post(r, k1, k2, k3):
            kr = m.load("sr", r) - m.load("hr", r) - (k1 - k3) + jnp.where(eye(r), 1.0, 0.0)
            ki = m.load("si", r) - m.load("hi", r) - (k1 + k2)
            a = m.load("or", r)
            b = m.load("oi", r)
            gr = kr * a - ki * b
            gi = kr * b + ki * a
            m.put(f"Gs{i}" if i == 4 else f"s{i % 2}", r, gr + gi)
            m.put(f"Gd{i}" if i == 4 else f"d{i % 2}", r, gr - gi)
            if 0 < i < 4:
                m.store(f"gs{i}", r, gr + gi)
                m.store(f"gd{i}", r, gr - gi)
            if i == 0:
                m.put("p0", r, gr * source(0))
                m.put("q0", r, gi * source(0))

        pieces(post, m.mm("Hs", "Sr"), m.mm("Hr", "Sa"), m.mm("Hi", "Sb"))

    def hop(i):
        pieces(lambda r, u, v: (m.put(f"u{i}", r, u), m.put(f"v{i}", r, v)), m.mm(f"s{i % 2}", f"V{i}"), m.mm(f"d{i % 2}", f"V{i}"))

    def names(i):
        return ("Gs4", "Gd4") if i == 4 else (f"s{i % 2}", f"d{i % 2}")

    def inflow(i):
        gamma = source(i)
        pieces(lambda r, y: m.put(f"C{i % 2}", r, y + jnp.where(eye(r), gamma, 0.0)), m.mm(f"Vt{i - 1}", f"U{i - 1}"))

    def dressed(i):
        s, d = names(i)
        C = f"C{i % 2}"
        pieces(lambda r, p: m.put(f"p{i % 2}", r, 0.5 * p), m.mm(d, C) + m.mm(s, C, True))
        pieces(lambda r, a, b: m.put(f"q{i % 2}", r, 0.5 * (a - b)), m.mm(s, C), m.mm(d, C, True))

    def lesser(i):
        s, d = names(i)

        def post(r, w):
            if i < 4:
                m.store(f"w{i}", r, w)
                m.put("Wl", r, w)
            else:
                m.put("W4", r, w)

        pieces(post, m.mm(f"p{i % 2}", d) + m.mm(f"q{i % 2}", s))

    def lesser_turned(i):
        pieces(lambda r, x: m.put("Wt", r, x), m.turned(f"w{i}"))

    def lesser_hop(i):
        pieces(lambda r, a, b: (m.put(f"U{i}", r, a), m.put(f"T{i}", r, b)), m.mm("Wl", f"V{i}"), m.mm("Wt", f"V{i}"))

    blocks[0].wait()
    scale(0)
    square(0)
    hops.wait()
    for i in range(4):
        pieces(lambda r, x: m.put(f"V{i}", r, x), coup[kind[i]])
        pieces(lambda r, x: m.put(f"Vt{i}", r, x), coup[kind[i]].T)
    green(0)
    hop(0)
    for i in range(1, 5):
        own_energy(i)
        if i > 1:
            dressed(i - 1)
        scale(i)
        lesser(i - 1)
        square(i)
        lesser_turned(i - 1)
        green(i)
        lesser_hop(i - 1)
        if i < 4:
            hop(i)
        inflow(i)
    steps = {i: back_products(m, i, weight, done) for i in (3, 2, 1)}
    dressed(4)
    steps[3][3]()
    lesser(4)
    steps[3][4]()
    steps[3][0]()
    steps[2][3]()
    steps[3][1]()
    steps[2][4]()
    steps[3][2]()
    hand_out(3, done, keep, send)
    steps[2][0]()
    steps[1][3]()
    steps[2][1]()
    steps[1][4]()
    steps[2][2]()
    hand_out(2, done, keep, send)


def backward_kernel(kept_pairs, kept_full, keep, send, pairs, full, done):
    m = Parts(pairs, full, kept_pairs, kept_full)
    weight = kept_full[KEPT_FULL.index("weight"), 0:1, :]
    for i in (1, 0):
        bond, density, report, _, _ = back_products(m, i, weight, done)
        bond()
        density()
        report()
        hand_out(i, done, keep, send)


def cost(products):
    return pl.CostEstimate(flops=products * 6 * N**3, bytes_accessed=8 * 2**20, transcendentals=0)


BLOCK = (16, 4, 16, N)


def forward(arrays):
    smem = pl.BlockSpec(memory_space=pltpu.SMEM)
    vmem = pl.BlockSpec(memory_space=pltpu.VMEM)
    hbm = pl.BlockSpec(memory_space=pltpu.HBM)
    return pl.pallas_call(
        forward_kernel,
        out_shape=(
            jax.ShapeDtypeStruct(BLOCK, f32),
            jax.ShapeDtypeStruct(BLOCK, f32),
            jax.ShapeDtypeStruct((len(KEPT), 2, N, N), bf16),
            jax.ShapeDtypeStruct((len(KEPT_FULL), N, N), f32),
        ),
        in_specs=[smem] * 4 + [hbm] * 8,
        out_specs=(vmem,) * 4,
        scratch_shapes=[
            pltpu.VMEM((56, 2, N, N), bf16),
            pltpu.VMEM((18, N, N), f32),
            pltpu.VMEM((4, 16, 16, N), f32),
            pltpu.SMEM((8,), f32),
            pltpu.SMEM((8,), f32),
            pltpu.SMEM((5,), f32),
            pltpu.SMEM((4,), jnp.int32),
            pltpu.VMEM((5, N), f32),
            pltpu.VMEM((5, N), f32),
            pltpu.VMEM((5, N, N), f32),
            pltpu.VMEM((3, N, N), f32),
            pltpu.SemaphoreType.DMA((12,)),
        ],
        compiler_params=pltpu.CompilerParams(vmem_limit_bytes=44 * 1024 * 1024),
        cost_estimate=cost(132),
    )(*arrays[:4], *[pltpu.with_memory_space_constraint(a, pltpu.HBM) for a in arrays[4:]])


def backward(kept_pairs, kept_full):
    vmem = pl.BlockSpec(memory_space=pltpu.VMEM)
    return pl.pallas_call(
        backward_kernel,
        out_shape=(jax.ShapeDtypeStruct(BLOCK, f32), jax.ShapeDtypeStruct(BLOCK, f32)),
        in_specs=[vmem] * 2,
        out_specs=(vmem,) * 2,
        scratch_shapes=[
            pltpu.VMEM((4, 2, N, N), bf16),
            pltpu.VMEM((2, N, N), f32),
            pltpu.VMEM((4, 16, 16, N), f32),
        ],
        compiler_params=pltpu.CompilerParams(vmem_limit_bytes=12 * 1024 * 1024),
        cost_estimate=cost(24),
    )(kept_pairs, kept_full)


def swapped(x, axes, partner):
    count = 1
    for a in axes:
        count *= lax.axis_size(a)
    return lax.ppermute(x, axes, [(i, partner(i)) for i in range(count)])


def over_core(x):
    return swapped(x, ("energy",), lambda i: i ^ 1)


def over_x(x, turn):
    return swapped(x, ("energy",), lambda i: i ^ (12 if (i & 1) ^ turn else 4))


def over_y(x, step):
    return swapped(x, ("layer",), lambda i: i ^ step)


def over_z(x):
    return swapped(x, ("energy",), lambda i: i ^ 2)


def to_one_block(keep, got):
    mine, other = keep, got
    count = 16
    for across in (lambda x: over_x(x, 0), lambda x: over_x(x, 1), lambda x: over_y(x, 1), over_z):
        count //= 2
        away = mine[count:] + other[count:]
        mine, other = mine[:count] + other[:count], across(away)
    return mine[0] + other[0]


def per_device(energies, momenta, energy_level, momentum_level, energy_table, momentum_table, onsite, broad, kdiag, fermi, couplings, bond_kind):
    keep_high, send_high, kept_pairs, kept_full = forward(
        (energies, momenta, energy_level, momentum_level, energy_table, momentum_table, fermi, bond_kind, broad, kdiag, onsite, couplings)
    )
    got_high = over_core(send_high)
    keep_low, send_low = backward(kept_pairs, kept_full)
    got_low = over_core(send_low)
    high = to_one_block(keep_high, got_high)
    low = to_one_block(keep_low, got_low)
    upper = lax.axis_index("layer") >= 2
    got = over_y(jnp.where(upper, low, high), 3)
    mine = jnp.where(upper, high, low) + got
    near, far, last = (swapped(mine, ("kpt",), lambda i, s=s: i ^ s) for s in (1, 2, 3))
    total = (mine + near) + (far + last)
    return total[None, :2], total[None, 2:]


def solution(mesh):
    return jax.shard_map(
        per_device,
        mesh=mesh,
        in_specs=(P(("energy", "layer")), P("kpt"), P(("energy", "layer")), P("kpt"), P(), P(), P(), P(), P(), P(), P(), P()),
        out_specs=(P("layer", None, "energy", None), P("layer", None, "energy", None)),
        check_vma=False,
    )
```

```python
import jax
import jax.numpy as jnp
from jax import lax
from jax.experimental import pallas as pl
from jax.experimental.pallas import tpu as pltpu
from jax.sharding import PartitionSpec as P


N = 256
CH = 32
f32 = jnp.float32
bf16 = jnp.bfloat16
KEPT = ("u0", "v0", "U0", "T0", "u1", "v1", "U1", "T1", "W2", "Gs2", "Gd2", "Gs1", "Gd1")
KEPT_FULL = ("w0", "w1", "weight")


def step_of(at, swap):
    first, second = at >> 1, at & 1
    plain = first ^ (3 * second)
    return plain ^ (swap * 2 * (first ^ second))


class Parts:
    def __init__(self, pairs, full, kept_pairs=None, kept_full=None):
        self.pairs, self.full = pairs, full
        self.at, self.full_at = {}, {}
        self.kept = {} if kept_pairs is None else {n: (kept_pairs, i) for i, n in enumerate(KEPT)}
        self.kept_full = {} if kept_full is None else {n: (kept_full, i) for i, n in enumerate(KEPT_FULL)}

    def pair(self, name):
        if name in self.kept:
            return self.kept[name]
        i = self.at.setdefault(name, len(self.at))
        assert i < self.pairs.shape[0]
        return self.pairs, i

    def whole(self, name):
        if name in self.kept_full:
            return self.kept_full[name]
        i = self.full_at.setdefault(name, len(self.full_at))
        assert i < self.full.shape[0]
        return self.full, i

    def put(self, name, r, x):
        ref, i = self.pair(name)
        high = x.astype(bf16)
        ref[i, 0, r, :] = high
        ref[i, 1, r, :] = (x - high.astype(f32)).astype(bf16)

    def store(self, name, r, x):
        ref, i = self.whole(name)
        ref[i, r, :] = x

    def load(self, name, r):
        ref, i = self.whole(name)
        return ref[i, r, :]

    def turned(self, name):
        ref, i = self.whole(name)
        return ref[i].T

    def mm(self, left, right, turn=False):
        a, i = self.pair(left)
        b, j = self.pair(right)
        contract = (((1,), (1 if turn else 0,)), ((), ()))

        def dot(x, y):
            return lax.dot_general(x, y, contract, preferred_element_type=f32)

        high = a[i, 0]
        return dot(high, b[j, 0]) + dot(high, b[j, 1]) + dot(a[i, 1], b[j, 0])


def pieces(post, *values):
    for c0 in range(0, N, CH):
        r = slice(c0, c0 + CH)
        post(r, *[v[r] for v in values])


def eye(r):
    rows = lax.broadcasted_iota(jnp.int32, (CH, N), 0) + r.start
    return rows == lax.broadcasted_iota(jnp.int32, (CH, N), 1)


def hand_out(layer, done, keep, send):
    energy = lax.axis_index("energy")
    core = energy & 1
    my_x, my_z = energy >> 2, (energy >> 1) & 1
    where_y = lax.axis_index("layer")
    y_at = (layer ^ (layer >> 1) ^ where_y ^ (where_y >> 1)) & 1
    for core_at, to in ((0, keep), (1, send)):
        turn = core ^ core_at
        for x_at in range(4):
            x_from = my_x ^ step_of(x_at, turn)
            for z_at in range(2):
                chunk = x_from * 4 + (my_z ^ z_at) * 2 + turn
                other = y_at * (2 - turn) + z_at * (1 + turn)
                spot = x_at * 4 + other if layer >= 2 else other * 4 + x_at
                for comp in range(4):
                    to[spot, comp] = done[comp, chunk]


def back_products(m, i, weight, done):
    u, v, U, T = f"u{i}", f"v{i}", f"U{i}", f"T{i}"
    W, Gs, Gd = f"W{i + 1}", f"Gs{i + 1}", f"Gd{i + 1}"

    def result(comp, r, x):
        for c0 in range(0, CH, 16):
            done[comp, (r.start + c0) // 16] = x[c0 : c0 + 16]

    def bond_re(r, a, b):
        result(2, r, weight * (0.5 * (a + b)))
        m.put("Yr", r, 0.25 * a + 0.5 * b)

    def bond_im(r, a, b, c, d):
        a, c = a - b, c - d
        result(3, r, weight * (0.5 * (a + c)))
        m.put("Yi", r, 0.25 * a + 0.5 * c)

    def bond():
        pieces(bond_re, m.mm(v, W) + m.mm(u, W, True), m.mm(U, Gs) + m.mm(T, Gd))
        pieces(bond_im, m.mm(u, W), m.mm(v, W, True), m.mm(U, Gd), m.mm(T, Gs))

    def new_w(r, a, b):
        w = m.load(f"w{i}", r) + a - b
        m.store("Wfull", r, w)
        if i:
            m.put(f"W{i}", r, w)

    def density():
        pieces(new_w, m.mm("Yr", v, True) + m.mm("Yi", u, True) + m.mm(u, "Yr", True), m.mm(v, "Yi", True))

    def dens(r, turned):
        a = m.load("Wfull", r)
        result(0, r, weight * (0.5 * (a + turned)))
        result(1, r, weight * (0.5 * (a - turned)))

    def report():
        pieces(dens, m.turned("Wfull"))

    def carry():
        pieces(lambda r, a: m.put("Qr", r, 0.5 * a), m.mm(u, Gd) + m.mm(v, Gs))
        pieces(lambda r, a, b: m.put("Qi", r, 0.5 * (a - b)), m.mm(u, Gs), m.mm(v, Gd))

    def spread():
        pieces(lambda r, a: m.put(f"Gs{i}", r, m.load(f"gs{i}", r) + a), m.mm("Qr", u, True) + m.mm("Qi", v, True))
        pieces(lambda r, a, b: m.put(f"Gd{i}", r, m.load(f"gd{i}", r) + a - b), m.mm("Qr", v, True), m.mm("Qi", u, True))

    return bond, density, report, carry, spread


def forward_kernel(*refs):
    arrays, (keep, send, kept_pairs, kept_full, pairs, full, done), local, sems = refs[4:12], refs[12:19], refs[19:27], refs[27]
    pe, pk, elev, mlev = refs[:4]
    etab, mtab, fermi, kind, broad, kdiag, onsite, coup = local
    small = [pltpu.make_async_copy(arrays[n], local[n], sems.at[n]) for n in range(6)]
    blocks = [pltpu.make_async_copy(arrays[6].at[n], onsite.at[n], sems.at[6 + n]) for n in range(5)]
    hops = pltpu.make_async_copy(arrays[7], coup, sems.at[11])
    for copy in small + blocks[:1] + [hops] + blocks[1:]:
        copy.start()
    m = Parts(pairs, full, kept_pairs, kept_full)
    for copy in small:
        copy.wait()
    e = pe[0]
    k = pk[0]
    weight = jnp.full((1, N), etab[elev[0]] * mtab[mlev[0]] * (1.0 / 256), f32)
    kept_full[KEPT_FULL.index("weight"), 0:8, :] = jnp.broadcast_to(weight, (8, N))

    def source(i):
        return broad[i : i + 1, :] * jax.nn.sigmoid(jnp.full((1, N), (fermi[i] - e) / 0.25, f32))

    def real_part(i, r):
        return m.load("mr", r) if i else onsite[0, r, :]

    def own_energy(i):
        def post(r, s, d):
            m.store("mr", r, onsite[i, r, :] + 0.5 * (s + d))
            m.store("mi", r, 0.5 * (s - d))

        blocks[i].wait()
        pieces(post, m.mm(f"Vt{i - 1}", f"u{i - 1}"), m.mm(f"Vt{i - 1}", f"v{i - 1}"))

    def scale(i):
        dr = jnp.zeros((1, N), f32)
        di = jnp.zeros((1, N), f32)
        for c0 in range(0, N, CH):
            r = slice(c0, c0 + CH)
            dr = dr + jnp.sum(jnp.where(eye(r), real_part(i, r), 0.0), axis=0, keepdims=True)
            if i:
                di = di + jnp.sum(jnp.where(eye(r), m.load("mi", r), 0.0), axis=0, keepdims=True)
        dr = e - k * kdiag[i : i + 1, :] - dr
        di = 0.5 * broad[i : i + 1, :] - di
        modulus = dr * dr + di * di
        zr = dr / modulus
        zi = -di / modulus
        size = jnp.sqrt(zr * zr + zi * zi)
        large = jnp.sqrt(0.5 * (size + jnp.abs(zr)))
        other = 0.5 * zi / large
        rr = jnp.where(zr >= 0.0, large, jnp.abs(other))
        ri = jnp.where(zr >= 0.0, other, jnp.where(zi < 0.0, -large, large))

        def post(r):
            mask = eye(r)
            cr = jnp.sum(jnp.where(mask, rr, 0.0), axis=1, keepdims=True)
            ci = jnp.sum(jnp.where(mask, ri, 0.0), axis=1, keepdims=True)
            a = cr * rr - ci * ri
            b = cr * ri + ci * rr
            m.store("or", r, a)
            m.store("oi", r, b)
            er = jnp.where(mask, 0.0, -real_part(i, r))
            if i:
                ei = jnp.where(mask, 0.0, -m.load("mi", r))
                hr, hi = er * a - ei * b, er * b + ei * a
            else:
                hr, hi = er * a, er * b
            m.store("hr", r, hr)
            m.store("hi", r, hi)
            m.put("Hr", r, hr)
            m.put("Hi", r, hi)
            m.put("Hs", r, hr + hi)

        pieces(post)

    def square():
        def post(r, a, b, c):
            m.store("sr", r, a - b)
            m.store("si", r, c - a - b)
            m.put("Sr", r, a - b)
            m.put("Sa", r, c - 2.0 * a)
            m.put("Sb", r, c - 2.0 * b)

        pieces(post, m.mm("Hr", "Hr"), m.mm("Hi", "Hi"), m.mm("Hs", "Hs"))

    def green(i):
        def post(r, k1, k2, k3):
            kr = m.load("sr", r) - m.load("hr", r) - (k1 - k3) + jnp.where(eye(r), 1.0, 0.0)
            ki = m.load("si", r) - m.load("hi", r) - (k1 + k2)
            a = m.load("or", r)
            b = m.load("oi", r)
            gr = kr * a - ki * b
            gi = kr * b + ki * a
            m.put(f"Gs{i}" if i == 4 else f"s{i % 2}", r, gr + gi)
            m.put(f"Gd{i}" if i == 4 else f"d{i % 2}", r, gr - gi)
            if 0 < i < 4:
                m.store(f"gs{i}", r, gr + gi)
                m.store(f"gd{i}", r, gr - gi)
            if i == 0:
                m.put("p0", r, gr * source(0))
                m.put("q0", r, gi * source(0))

        pieces(post, m.mm("Hs", "Sr"), m.mm("Hr", "Sa"), m.mm("Hi", "Sb"))

    def hop(i):
        pieces(lambda r, u, v: (m.put(f"u{i}", r, u), m.put(f"v{i}", r, v)), m.mm(f"s{i % 2}", f"V{i}"), m.mm(f"d{i % 2}", f"V{i}"))

    def names(i):
        return ("Gs4", "Gd4") if i == 4 else (f"s{i % 2}", f"d{i % 2}")

    def inflow(i):
        gamma = source(i)
        pieces(lambda r, y: m.put(f"C{i % 2}", r, y + jnp.where(eye(r), gamma, 0.0)), m.mm(f"Vt{i - 1}", f"U{i - 1}"))

    def dressed(i):
        s, d = names(i)
        C = f"C{i % 2}"
        pieces(lambda r, p: m.put(f"p{i % 2}", r, 0.5 * p), m.mm(d, C) + m.mm(s, C, True))
        pieces(lambda r, a, b: m.put(f"q{i % 2}", r, 0.5 * (a - b)), m.mm(s, C), m.mm(d, C, True))

    def lesser(i):
        s, d = names(i)

        def post(r, w):
            if i < 4:
                m.store(f"w{i}", r, w)
                m.put("Wl", r, w)
            else:
                m.put("W4", r, w)

        pieces(post, m.mm(f"p{i % 2}", d) + m.mm(f"q{i % 2}", s))

    def lesser_turned(i):
        pieces(lambda r, x: m.put("Wt", r, x), m.turned(f"w{i}"))

    def lesser_hop(i):
        pieces(lambda r, a, b: (m.put(f"U{i}", r, a), m.put(f"T{i}", r, b)), m.mm("Wl", f"V{i}"), m.mm("Wt", f"V{i}"))

    blocks[0].wait()
    scale(0)
    square()
    hops.wait()
    for i in range(4):
        pieces(lambda r, x: m.put(f"V{i}", r, x), coup[kind[i]])
        pieces(lambda r, x: m.put(f"Vt{i}", r, x), coup[kind[i]].T)
    green(0)
    hop(0)
    for i in range(1, 5):
        own_energy(i)
        if i > 1:
            dressed(i - 1)
        scale(i)
        lesser(i - 1)
        square()
        lesser_turned(i - 1)
        green(i)
        lesser_hop(i - 1)
        if i < 4:
            hop(i)
        inflow(i)
    steps = {i: back_products(m, i, weight, done) for i in (3, 2, 1)}
    dressed(4)
    steps[3][3]()
    lesser(4)
    steps[3][4]()
    steps[3][0]()
    steps[2][3]()
    steps[3][1]()
    steps[2][4]()
    steps[3][2]()
    hand_out(3, done, keep, send)
    steps[2][0]()
    steps[1][3]()
    steps[2][1]()
    steps[1][4]()
    steps[2][2]()
    hand_out(2, done, keep, send)


def third_kernel(kept_pairs, kept_full, next_pair, done, pairs, full):
    m = Parts(pairs, full, kept_pairs, kept_full)
    m.kept["W1"] = (next_pair, 0)
    for step in back_products(m, 1, kept_full[KEPT_FULL.index("weight"), 0:1, :], done)[:3]:
        step()


def last_kernel(kept_pairs, kept_full, next_pair, done_before, keep, send, pairs, full, done):
    m = Parts(pairs, full, kept_pairs, kept_full)
    m.kept["W1"] = (next_pair, 0)
    hand_out(1, done_before, keep, send)
    for step in back_products(m, 0, kept_full[KEPT_FULL.index("weight"), 0:1, :], done)[:3]:
        step()
    hand_out(0, done, keep, send)


def cost(products):
    return pl.CostEstimate(flops=products * 6 * N**3, bytes_accessed=8 * 2**20, transcendentals=0)


BLOCK = (16, 4, 16, N)


def forward(arrays):
    smem = pl.BlockSpec(memory_space=pltpu.SMEM)
    vmem = pl.BlockSpec(memory_space=pltpu.VMEM)
    hbm = pl.BlockSpec(memory_space=pltpu.HBM)
    return pl.pallas_call(
        forward_kernel,
        out_shape=(
            jax.ShapeDtypeStruct(BLOCK, f32),
            jax.ShapeDtypeStruct(BLOCK, f32),
            jax.ShapeDtypeStruct((len(KEPT), 2, N, N), bf16),
            jax.ShapeDtypeStruct((len(KEPT_FULL), N, N), f32),
        ),
        in_specs=[smem] * 4 + [hbm] * 8,
        out_specs=(vmem,) * 4,
        scratch_shapes=[
            pltpu.VMEM((56, 2, N, N), bf16),
            pltpu.VMEM((18, N, N), f32),
            pltpu.VMEM((4, 16, 16, N), f32),
            pltpu.SMEM((8,), f32),
            pltpu.SMEM((8,), f32),
            pltpu.SMEM((5,), f32),
            pltpu.SMEM((4,), jnp.int32),
            pltpu.VMEM((5, N), f32),
            pltpu.VMEM((5, N), f32),
            pltpu.VMEM((5, N, N), f32),
            pltpu.VMEM((3, N, N), f32),
            pltpu.SemaphoreType.DMA((12,)),
        ],
        compiler_params=pltpu.CompilerParams(vmem_limit_bytes=44 * 1024 * 1024),
        cost_estimate=cost(132),
    )(*arrays[:4], *[pltpu.with_memory_space_constraint(a, pltpu.HBM) for a in arrays[4:]])


def third(kept_pairs, kept_full):
    vmem = pl.BlockSpec(memory_space=pltpu.VMEM)
    return pl.pallas_call(
        third_kernel,
        out_shape=(jax.ShapeDtypeStruct((1, 2, N, N), bf16), jax.ShapeDtypeStruct((4, 16, 16, N), f32)),
        in_specs=[vmem] * 2,
        out_specs=(vmem,) * 2,
        scratch_shapes=[pltpu.VMEM((3, 2, N, N), bf16), pltpu.VMEM((1, N, N), f32)],
        compiler_params=pltpu.CompilerParams(vmem_limit_bytes=12 * 1024 * 1024),
        cost_estimate=cost(12),
    )(kept_pairs, kept_full)


def last(kept_pairs, kept_full, next_pair, done_before):
    vmem = pl.BlockSpec(memory_space=pltpu.VMEM)
    return pl.pallas_call(
        last_kernel,
        out_shape=(jax.ShapeDtypeStruct(BLOCK, f32), jax.ShapeDtypeStruct(BLOCK, f32)),
        in_specs=[vmem] * 4,
        out_specs=(vmem,) * 2,
        scratch_shapes=[
            pltpu.VMEM((3, 2, N, N), bf16),
            pltpu.VMEM((1, N, N), f32),
            pltpu.VMEM((4, 16, 16, N), f32),
        ],
        compiler_params=pltpu.CompilerParams(vmem_limit_bytes=12 * 1024 * 1024),
        cost_estimate=cost(12),
    )(kept_pairs, kept_full, next_pair, done_before)


def swapped(x, axes, partner):
    count = 1
    for a in axes:
        count *= lax.axis_size(a)
    return lax.ppermute(x, axes, [(i, partner(i)) for i in range(count)])


def over_core(x):
    return swapped(x, ("energy",), lambda i: i ^ 1)


def over_x(x, turn):
    return swapped(x, ("energy",), lambda i: i ^ (12 if (i & 1) ^ turn else 4))


def over_y(x, step):
    return swapped(x, ("layer",), lambda i: i ^ step)


def over_rest(x, turn):
    return swapped(x, ("energy", "layer"), lambda i: i ^ (8 if ((i >> 2) & 1) ^ turn else 1))


def halves(mine, other):
    count = mine.shape[0] // 2
    return mine[:count] + other[:count], mine[count:] + other[count:]


def per_device(energies, momenta, energy_level, momentum_level, energy_table, momentum_table, onsite, broad, kdiag, fermi, couplings, bond_kind):
    keep_high, send_high, kept_pairs, kept_full = forward(
        (energies, momenta, energy_level, momentum_level, energy_table, momentum_table, fermi, bond_kind, broad, kdiag, onsite, couplings)
    )
    got_high = over_core(send_high)
    next_pair, done = third(kept_pairs, kept_full)
    high, away_high = halves(keep_high, got_high)
    high, away_high, next_pair, done = lax.optimization_barrier((high, away_high, next_pair, done))
    got_high = over_x(away_high, 0)
    keep_low, send_low = last(kept_pairs, kept_full, next_pair, done)
    low, got_low = keep_low, over_core(send_low)
    for step in range(4):
        if step:
            high, away_high = halves(high, got_high)
            got_high = over_x(away_high, 1) if step == 1 else over_rest(away_high, step - 2)
        low, away_low = halves(low, got_low)
        got_low = over_rest(away_low, step) if step < 2 else over_x(away_low, step - 2)
    high = high[0] + got_high[0]
    low = low[0] + got_low[0]
    upper = lax.axis_index("layer") >= 2
    got = over_y(jnp.where(upper, low, high), 3)
    mine = jnp.where(upper, high, low) + got
    near, far, both = (swapped(mine, ("kpt",), lambda i, s=s: i ^ s) for s in (1, 2, 3))
    total = (mine + near) + (far + both)
    return total[None, :2], total[None, 2:]


def solution(mesh):
    return jax.shard_map(
        per_device,
        mesh=mesh,
        in_specs=(P(("energy", "layer")), P("kpt"), P(("energy", "layer")), P("kpt"), P(), P(), P(), P(), P(), P(), P(), P()),
        out_specs=(P("layer", None, "energy", None), P("layer", None, "energy", None)),
        check_vma=False,
    )
```

```python
import jax
import jax.numpy as jnp
from jax import lax
from jax.experimental import pallas as pl
from jax.experimental.pallas import tpu as pltpu
from jax.sharding import PartitionSpec as P


N = 256
CH = 32
f32 = jnp.float32
bf16 = jnp.bfloat16
KEPT = ("u0", "v0", "U0", "T0", "u1", "v1", "U1", "T1", "W2", "Gs2", "Gd2", "Gs1", "Gd1")
KEPT_FULL = ("w0", "w1", "weight")


def step_of(at, swap):
    first, second = at >> 1, at & 1
    plain = first ^ (3 * second)
    return plain ^ (swap * 2 * (first ^ second))


class Parts:
    def __init__(self, pairs, full, kept_pairs=None, kept_full=None):
        self.pairs, self.full = pairs, full
        self.at, self.full_at = {}, {}
        self.kept = {} if kept_pairs is None else {n: (kept_pairs, i) for i, n in enumerate(KEPT)}
        self.kept_full = {} if kept_full is None else {n: (kept_full, i) for i, n in enumerate(KEPT_FULL)}

    def pair(self, name):
        if name in self.kept:
            return self.kept[name]
        i = self.at.setdefault(name, len(self.at))
        assert i < self.pairs.shape[0]
        return self.pairs, i

    def whole(self, name):
        if name in self.kept_full:
            return self.kept_full[name]
        i = self.full_at.setdefault(name, len(self.full_at))
        assert i < self.full.shape[0]
        return self.full, i

    def put(self, name, r, x):
        ref, i = self.pair(name)
        high = x.astype(bf16)
        ref[i, 0, r, :] = high
        ref[i, 1, r, :] = (x - high.astype(f32)).astype(bf16)

    def store(self, name, r, x):
        ref, i = self.whole(name)
        ref[i, r, :] = x

    def load(self, name, r):
        ref, i = self.whole(name)
        return ref[i, r, :]

    def turned(self, name):
        ref, i = self.whole(name)
        return ref[i].T

    def mm(self, left, right, turn=False):
        a, i = self.pair(left)
        b, j = self.pair(right)
        contract = (((1,), (1 if turn else 0,)), ((), ()))

        def dot(x, y):
            return lax.dot_general(x, y, contract, preferred_element_type=f32)

        high = a[i, 0]
        return dot(high, b[j, 0]) + dot(high, b[j, 1]) + dot(a[i, 1], b[j, 0])


def pieces(post, *values):
    for c0 in range(0, N, CH):
        r = slice(c0, c0 + CH)
        post(r, *[v[r] for v in values])


def eye(r):
    rows = lax.broadcasted_iota(jnp.int32, (CH, N), 0) + r.start
    return rows == lax.broadcasted_iota(jnp.int32, (CH, N), 1)


def hand_out(layer, done, keep, send):
    energy = lax.axis_index("energy")
    core = energy & 1
    my_x, my_z = energy >> 2, (energy >> 1) & 1
    where_y = lax.axis_index("layer")
    y_at = (layer ^ (layer >> 1) ^ where_y ^ (where_y >> 1)) & 1
    for core_at, to in ((0, keep), (1, send)):
        turn = core ^ core_at
        for x_at in range(4):
            x_from = my_x ^ step_of(x_at, turn)
            for z_at in range(2):
                chunk = x_from * 4 + (my_z ^ z_at) * 2 + turn
                if layer >= 2:
                    spot = (y_at * (2 - turn) + z_at * (1 + turn)) * 4 + x_at
                else:
                    spot = (x_at >> 1) * 4 + (x_at & 1) * (2 - turn) + z_at * (1 + turn)
                for comp in range(4):
                    to[spot, comp] = done[comp, chunk]


def back_products(m, i, weight, done):
    u, v, U, T = f"u{i}", f"v{i}", f"U{i}", f"T{i}"
    W, Gs, Gd = f"W{i + 1}", f"Gs{i + 1}", f"Gd{i + 1}"

    def result(comp, r, x):
        for c0 in range(0, CH, 16):
            done[comp, (r.start + c0) // 16] = x[c0 : c0 + 16]

    def bond_re(r, a, b):
        result(2, r, weight * (0.5 * (a + b)))
        m.put("Yr", r, 0.25 * a + 0.5 * b)

    def bond_im(r, a, b, c, d):
        a, c = a - b, c - d
        result(3, r, weight * (0.5 * (a + c)))
        m.put("Yi", r, 0.25 * a + 0.5 * c)

    def bond():
        pieces(bond_re, m.mm(v, W) + m.mm(u, W, True), m.mm(U, Gs) + m.mm(T, Gd))
        pieces(bond_im, m.mm(u, W), m.mm(v, W, True), m.mm(U, Gd), m.mm(T, Gs))

    def new_w(r, a, b):
        w = m.load(f"w{i}", r) + a - b
        m.store("Wfull", r, w)
        if i:
            m.put(f"W{i}", r, w)

    def density():
        pieces(new_w, m.mm("Yr", v, True) + m.mm("Yi", u, True) + m.mm(u, "Yr", True), m.mm(v, "Yi", True))

    def dens(r, turned):
        a = m.load("Wfull", r)
        result(0, r, weight * (0.5 * (a + turned)))
        result(1, r, weight * (0.5 * (a - turned)))

    def report():
        pieces(dens, m.turned("Wfull"))

    def carry():
        pieces(lambda r, a: m.put("Qr", r, 0.5 * a), m.mm(u, Gd) + m.mm(v, Gs))
        pieces(lambda r, a, b: m.put("Qi", r, 0.5 * (a - b)), m.mm(u, Gs), m.mm(v, Gd))

    def spread():
        pieces(lambda r, a: m.put(f"Gs{i}", r, m.load(f"gs{i}", r) + a), m.mm("Qr", u, True) + m.mm("Qi", v, True))
        pieces(lambda r, a, b: m.put(f"Gd{i}", r, m.load(f"gd{i}", r) + a - b), m.mm("Qr", v, True), m.mm("Qi", u, True))

    return bond, density, report, carry, spread


def forward_kernel(*refs):
    arrays, (keep, send, kept_pairs, kept_full, sides, pairs, full, done), local, sems = refs[4:12], refs[12:20], refs[20:28], refs[28]
    pe, pk, elev, mlev = refs[:4]
    etab, mtab, fermi, kind, broad, kdiag, onsite, coup = local
    small = [pltpu.make_async_copy(arrays[n], local[n], sems.at[n]) for n in range(6)]
    blocks = [pltpu.make_async_copy(arrays[6].at[n], onsite.at[n], sems.at[6 + n]) for n in range(5)]
    hops = pltpu.make_async_copy(arrays[7], coup, sems.at[11])
    for copy in small + blocks[:1] + [hops] + blocks[1:]:
        copy.start()
    m = Parts(pairs, full, kept_pairs, kept_full)
    where = lax.axis_index("layer")
    sides[0] = jnp.full((16, N), (((where ^ (where >> 1)) & 1) == 1).astype(f32))
    sides[1] = jnp.full((16, N), (where >= 2).astype(f32))
    for copy in small:
        copy.wait()
    e = pe[0]
    k = pk[0]
    weight = jnp.full((1, N), etab[elev[0]] * mtab[mlev[0]] * (1.0 / 256), f32)
    kept_full[KEPT_FULL.index("weight"), 0:8, :] = jnp.broadcast_to(weight, (8, N))

    def source(i):
        return broad[i : i + 1, :] * jax.nn.sigmoid(jnp.full((1, N), (fermi[i] - e) / 0.25, f32))

    def real_part(i, r):
        return m.load("mr", r) if i else onsite[0, r, :]

    def own_energy(i):
        def post(r, s, d):
            m.store("mr", r, onsite[i, r, :] + 0.5 * (s + d))
            m.store("mi", r, 0.5 * (s - d))

        blocks[i].wait()
        pieces(post, m.mm(f"Vt{i - 1}", f"u{i - 1}"), m.mm(f"Vt{i - 1}", f"v{i - 1}"))

    def scale(i):
        dr = jnp.zeros((1, N), f32)
        di = jnp.zeros((1, N), f32)
        for c0 in range(0, N, CH):
            r = slice(c0, c0 + CH)
            dr = dr + jnp.sum(jnp.where(eye(r), real_part(i, r), 0.0), axis=0, keepdims=True)
            if i:
                di = di + jnp.sum(jnp.where(eye(r), m.load("mi", r), 0.0), axis=0, keepdims=True)
        dr = e - k * kdiag[i : i + 1, :] - dr
        di = 0.5 * broad[i : i + 1, :] - di
        modulus = dr * dr + di * di
        zr = dr / modulus
        zi = -di / modulus
        size = jnp.sqrt(zr * zr + zi * zi)
        large = jnp.sqrt(0.5 * (size + jnp.abs(zr)))
        other = 0.5 * zi / large
        rr = jnp.where(zr >= 0.0, large, jnp.abs(other))
        ri = jnp.where(zr >= 0.0, other, jnp.where(zi < 0.0, -large, large))

        def post(r):
            mask = eye(r)
            cr = jnp.sum(jnp.where(mask, rr, 0.0), axis=1, keepdims=True)
            ci = jnp.sum(jnp.where(mask, ri, 0.0), axis=1, keepdims=True)
            a = cr * rr - ci * ri
            b = cr * ri + ci * rr
            m.store("or", r, a)
            m.store("oi", r, b)
            er = jnp.where(mask, 0.0, -real_part(i, r))
            if i:
                ei = jnp.where(mask, 0.0, -m.load("mi", r))
                hr, hi = er * a - ei * b, er * b + ei * a
            else:
                hr, hi = er * a, er * b
            m.store("hr", r, hr)
            m.store("hi", r, hi)
            m.put("Hr", r, hr)
            m.put("Hi", r, hi)
            m.put("Hs", r, hr + hi)

        pieces(post)

    def square():
        def post(r, a, b, c):
            m.store("sr", r, a - b)
            m.store("si", r, c - a - b)
            m.put("Sr", r, a - b)
            m.put("Sa", r, c - 2.0 * a)
            m.put("Sb", r, c - 2.0 * b)

        pieces(post, m.mm("Hr", "Hr"), m.mm("Hi", "Hi"), m.mm("Hs", "Hs"))

    def green(i):
        def post(r, k1, k2, k3):
            kr = m.load("sr", r) - m.load("hr", r) - (k1 - k3) + jnp.where(eye(r), 1.0, 0.0)
            ki = m.load("si", r) - m.load("hi", r) - (k1 + k2)
            a = m.load("or", r)
            b = m.load("oi", r)
            gr = kr * a - ki * b
            gi = kr * b + ki * a
            m.put(f"Gs{i}" if i == 4 else f"s{i % 2}", r, gr + gi)
            m.put(f"Gd{i}" if i == 4 else f"d{i % 2}", r, gr - gi)
            if 0 < i < 4:
                m.store(f"gs{i}", r, gr + gi)
                m.store(f"gd{i}", r, gr - gi)
            if i == 0:
                m.put("p0", r, gr * source(0))
                m.put("q0", r, gi * source(0))

        pieces(post, m.mm("Hs", "Sr"), m.mm("Hr", "Sa"), m.mm("Hi", "Sb"))

    def hop(i):
        pieces(lambda r, u, v: (m.put(f"u{i}", r, u), m.put(f"v{i}", r, v)), m.mm(f"s{i % 2}", f"V{i}"), m.mm(f"d{i % 2}", f"V{i}"))

    def names(i):
        return ("Gs4", "Gd4") if i == 4 else (f"s{i % 2}", f"d{i % 2}")

    def inflow(i):
        gamma = source(i)
        pieces(lambda r, y: m.put(f"C{i % 2}", r, y + jnp.where(eye(r), gamma, 0.0)), m.mm(f"Vt{i - 1}", f"U{i - 1}"))

    def dressed(i):
        s, d = names(i)
        C = f"C{i % 2}"
        pieces(lambda r, p: m.put(f"p{i % 2}", r, 0.5 * p), m.mm(d, C) + m.mm(s, C, True))
        pieces(lambda r, a, b: m.put(f"q{i % 2}", r, 0.5 * (a - b)), m.mm(s, C), m.mm(d, C, True))

    def lesser(i):
        s, d = names(i)

        def post(r, w):
            if i < 4:
                m.store(f"w{i}", r, w)
                m.put("Wl", r, w)
            else:
                m.put("W4", r, w)

        pieces(post, m.mm(f"p{i % 2}", d) + m.mm(f"q{i % 2}", s))

    def lesser_turned(i):
        pieces(lambda r, x: m.put("Wt", r, x), m.turned(f"w{i}"))

    def lesser_hop(i):
        pieces(lambda r, a, b: (m.put(f"U{i}", r, a), m.put(f"T{i}", r, b)), m.mm("Wl", f"V{i}"), m.mm("Wt", f"V{i}"))

    blocks[0].wait()
    scale(0)
    square()
    hops.wait()
    for i in range(4):
        pieces(lambda r, x: m.put(f"V{i}", r, x), coup[kind[i]])
        pieces(lambda r, x: m.put(f"Vt{i}", r, x), coup[kind[i]].T)
    green(0)
    hop(0)
    for i in range(1, 5):
        own_energy(i)
        if i > 1:
            dressed(i - 1)
        scale(i)
        lesser(i - 1)
        square()
        lesser_turned(i - 1)
        green(i)
        lesser_hop(i - 1)
        if i < 4:
            hop(i)
        inflow(i)
    steps = {i: back_products(m, i, weight, done) for i in (3, 2, 1)}
    dressed(4)
    steps[3][3]()
    lesser(4)
    steps[3][4]()
    steps[3][0]()
    steps[2][3]()
    steps[3][1]()
    steps[2][4]()
    steps[3][2]()
    hand_out(3, done, keep, send)
    steps[2][0]()
    steps[1][3]()
    steps[2][1]()
    steps[1][4]()
    steps[2][2]()
    hand_out(2, done, keep, send)


def third_kernel(kept_pairs, kept_full, next_pair, keep, send, pairs, full, done):
    m = Parts(pairs, full, kept_pairs, kept_full)
    m.kept["W1"] = (next_pair, 0)
    for step in back_products(m, 1, kept_full[KEPT_FULL.index("weight"), 0:1, :], done)[:3]:
        step()
    hand_out(1, done, keep, send)


def last_kernel(kept_pairs, kept_full, next_pair, keep, send, pairs, full, done):
    m = Parts(pairs, full, kept_pairs, kept_full)
    m.kept["W1"] = (next_pair, 0)
    for step in back_products(m, 0, kept_full[KEPT_FULL.index("weight"), 0:1, :], done)[:3]:
        step()
    hand_out(0, done, keep, send)


def cost(products):
    return pl.CostEstimate(flops=products * 6 * N**3, bytes_accessed=8 * 2**20, transcendentals=0)


BLOCK = (16, 4, 16, N)
HALF_BLOCK = (8, 4, 16, N)


def forward(arrays):
    smem = pl.BlockSpec(memory_space=pltpu.SMEM)
    vmem = pl.BlockSpec(memory_space=pltpu.VMEM)
    hbm = pl.BlockSpec(memory_space=pltpu.HBM)
    return pl.pallas_call(
        forward_kernel,
        out_shape=(
            jax.ShapeDtypeStruct(BLOCK, f32),
            jax.ShapeDtypeStruct(BLOCK, f32),
            jax.ShapeDtypeStruct((len(KEPT), 2, N, N), bf16),
            jax.ShapeDtypeStruct((len(KEPT_FULL), N, N), f32),
            jax.ShapeDtypeStruct((2, 16, N), f32),
        ),
        in_specs=[smem] * 4 + [hbm] * 8,
        out_specs=(vmem,) * 5,
        scratch_shapes=[
            pltpu.VMEM((56, 2, N, N), bf16),
            pltpu.VMEM((18, N, N), f32),
            pltpu.VMEM((4, 16, 16, N), f32),
            pltpu.SMEM((8,), f32),
            pltpu.SMEM((8,), f32),
            pltpu.SMEM((5,), f32),
            pltpu.SMEM((4,), jnp.int32),
            pltpu.VMEM((5, N), f32),
            pltpu.VMEM((5, N), f32),
            pltpu.VMEM((5, N, N), f32),
            pltpu.VMEM((3, N, N), f32),
            pltpu.SemaphoreType.DMA((12,)),
        ],
        compiler_params=pltpu.CompilerParams(vmem_limit_bytes=32 * 1024 * 1024),
        cost_estimate=cost(132),
    )(*arrays[:4], *[pltpu.with_memory_space_constraint(a, pltpu.HBM) for a in arrays[4:]])


def third(kept_pairs, kept_full):
    vmem = pl.BlockSpec(memory_space=pltpu.VMEM)
    return pl.pallas_call(
        third_kernel,
        out_shape=(
            jax.ShapeDtypeStruct((1, 2, N, N), bf16),
            jax.ShapeDtypeStruct(HALF_BLOCK, f32),
            jax.ShapeDtypeStruct(HALF_BLOCK, f32),
        ),
        in_specs=[vmem] * 2,
        out_specs=(vmem,) * 3,
        scratch_shapes=[
            pltpu.VMEM((3, 2, N, N), bf16),
            pltpu.VMEM((1, N, N), f32),
            pltpu.VMEM((4, 16, 16, N), f32),
        ],
        compiler_params=pltpu.CompilerParams(vmem_limit_bytes=12 * 1024 * 1024),
        cost_estimate=cost(12),
    )(kept_pairs, kept_full)


def last(kept_pairs, kept_full, next_pair):
    vmem = pl.BlockSpec(memory_space=pltpu.VMEM)
    return pl.pallas_call(
        last_kernel,
        out_shape=(jax.ShapeDtypeStruct(HALF_BLOCK, f32), jax.ShapeDtypeStruct(HALF_BLOCK, f32)),
        in_specs=[vmem] * 3,
        out_specs=(vmem,) * 2,
        scratch_shapes=[
            pltpu.VMEM((3, 2, N, N), bf16),
            pltpu.VMEM((1, N, N), f32),
            pltpu.VMEM((4, 16, 16, N), f32),
        ],
        compiler_params=pltpu.CompilerParams(vmem_limit_bytes=12 * 1024 * 1024),
        cost_estimate=cost(12),
    )(kept_pairs, kept_full, next_pair)


def swapped(x, axes, partner):
    count = 1
    for a in axes:
        count *= lax.axis_size(a)
    return lax.ppermute(x, axes, [(i, partner(i)) for i in range(count)])


def over_core(x):
    return swapped(x, ("energy",), lambda i: i ^ 1)


def over_x(x, turn):
    return swapped(x, ("energy",), lambda i: i ^ (12 if (i & 1) ^ turn else 4))


def over_y(x, step):
    return swapped(x, ("layer",), lambda i: i ^ step)


def over_rest(x, turn):
    return swapped(x, ("energy", "layer"), lambda i: i ^ (8 if ((i >> 2) & 1) ^ turn else 1))


def over_mixed(x, turn):
    return swapped(x, ("energy",), lambda i: i ^ ((12, 4)[i & 1] if (i & 1) == turn else 2))


def halves(mine, other):
    count = mine.shape[0] // 2
    return mine[:count] + other[:count], mine[count:] + other[count:]


def per_device(energies, momenta, energy_level, momentum_level, energy_table, momentum_table, onsite, broad, kdiag, fermi, couplings, bond_kind):
    keep_high, send_high, kept_pairs, kept_full, sides = forward(
        (energies, momenta, energy_level, momentum_level, energy_table, momentum_table, fermi, bond_kind, broad, kdiag, onsite, couplings)
    )
    got_high = over_core(send_high)
    next_pair, keep_1, send_1 = third(kept_pairs, kept_full)
    high, away_high = halves(keep_high, got_high)
    high, away_high, next_pair, send_1 = lax.optimization_barrier((high, away_high, next_pair, send_1))
    got_high = over_rest(away_high, 0)
    got_1 = over_core(send_1)
    keep_0, send_0 = last(kept_pairs, kept_full, next_pair)
    got_0 = over_core(send_0)
    low_1, low_0 = keep_1, keep_0
    for step in range(3):
        low_1, away_1 = halves(low_1, got_1)
        got_1 = over_mixed(away_1, step - 1) if step else over_x(away_1, 0)
        low_0, away_0 = halves(low_0, got_0)
        got_0 = over_mixed(away_0, step - 1) if step else over_x(away_0, 0)
        high, away_high = halves(high, got_high)
        got_high = over_x(away_high, step - 1) if step else over_rest(away_high, 1)
    high = high[0] + got_high[0]
    low_1 = low_1[0] + got_1[0]
    low_0 = low_0[0] + got_0[0]
    odd, upper = sides[0] > 0.5, sides[1] > 0.5
    low = jnp.where(odd, low_1, low_0) + over_y(jnp.where(odd, low_0, low_1), 1)
    got = over_y(jnp.where(upper, low, high), 3)
    mine = jnp.where(upper, high, low) + got
    near, far, both = (swapped(mine, ("kpt",), lambda i, s=s: i ^ s) for s in (1, 2, 3))
    total = (mine + near) + (far + both)
    return total[None, :2], total[None, 2:]


def solution(mesh):
    return jax.shard_map(
        per_device,
        mesh=mesh,
        in_specs=(P(("energy", "layer")), P("kpt"), P(("energy", "layer")), P("kpt"), P(), P(), P(), P(), P(), P(), P(), P()),
        out_specs=(P("layer", None, "energy", None), P("layer", None, "energy", None)),
        check_vma=False,
    )
```

```python
import jax
import jax.numpy as jnp
from jax import lax
from jax.experimental import pallas as pl
from jax.experimental.pallas import tpu as pltpu
from jax.sharding import PartitionSpec as P


N = 256
CH = 32
f32 = jnp.float32
bf16 = jnp.bfloat16
KEPT = ("u0", "v0", "U0", "T0", "u1", "v1", "U1", "T1", "W2", "Gs2", "Gd2", "Gs1", "Gd1")
KEPT_FULL = ("w0", "w1", "weight")


def step_of(at, swap):
    first, second = at >> 1, at & 1
    plain = first ^ (3 * second)
    return plain ^ (swap * 2 * (first ^ second))


class Parts:
    def __init__(self, pairs, full, kept_pairs=None, kept_full=None):
        self.pairs, self.full = pairs, full
        self.at, self.full_at = {}, {}
        self.kept = {} if kept_pairs is None else {n: (kept_pairs, i) for i, n in enumerate(KEPT)}
        self.kept_full = {} if kept_full is None else {n: (kept_full, i) for i, n in enumerate(KEPT_FULL)}

    def pair(self, name):
        if name in self.kept:
            return self.kept[name]
        i = self.at.setdefault(name, len(self.at))
        assert i < self.pairs.shape[0]
        return self.pairs, i

    def whole(self, name):
        if name in self.kept_full:
            return self.kept_full[name]
        i = self.full_at.setdefault(name, len(self.full_at))
        assert i < self.full.shape[0]
        return self.full, i

    def put(self, name, r, x):
        ref, i = self.pair(name)
        high = x.astype(bf16)
        ref[i, 0, r, :] = high
        ref[i, 1, r, :] = (x - high.astype(f32)).astype(bf16)

    def store(self, name, r, x):
        ref, i = self.whole(name)
        ref[i, r, :] = x

    def load(self, name, r):
        ref, i = self.whole(name)
        return ref[i, r, :]

    def turned(self, name):
        ref, i = self.whole(name)
        return ref[i].T

    def mm(self, left, right, turn=False):
        a, i = self.pair(left)
        b, j = self.pair(right)
        contract = (((1,), (1 if turn else 0,)), ((), ()))

        def dot(x, y):
            return lax.dot_general(x, y, contract, preferred_element_type=f32)

        high = a[i, 0]
        return dot(high, b[j, 0]) + dot(high, b[j, 1]) + dot(a[i, 1], b[j, 0])


def pieces(post, *values):
    for c0 in range(0, N, CH):
        r = slice(c0, c0 + CH)
        post(r, *[v[r] for v in values])


def eye(r):
    rows = lax.broadcasted_iota(jnp.int32, (CH, N), 0) + r.start
    return rows == lax.broadcasted_iota(jnp.int32, (CH, N), 1)


def hand_out(layer, done, keep, send):
    energy = lax.axis_index("energy")
    core = energy & 1
    my_x, my_z = energy >> 2, (energy >> 1) & 1
    where_y = lax.axis_index("layer")
    y_at = (layer ^ (layer >> 1) ^ where_y ^ (where_y >> 1)) & 1
    for core_at, to in ((0, keep), (1, send)):
        turn = core ^ core_at
        for x_at in range(4):
            x_from = my_x ^ step_of(x_at, turn)
            for z_at in range(2):
                chunk = x_from * 4 + (my_z ^ z_at) * 2 + turn
                if layer >= 2:
                    spot = (y_at * (2 - turn) + z_at * (1 + turn)) * 4 + x_at
                else:
                    spot = (x_at >> 1) * 4 + (x_at & 1) * (2 - turn) + z_at * (1 + turn)
                for comp in range(4):
                    to[spot, comp] = done[comp, chunk]


def back_products(m, i, weight, done):
    u, v, U, T = f"u{i}", f"v{i}", f"U{i}", f"T{i}"
    W, Gs, Gd = f"W{i + 1}", f"Gs{i + 1}", f"Gd{i + 1}"

    def result(comp, r, x):
        for c0 in range(0, CH, 16):
            done[comp, (r.start + c0) // 16] = x[c0 : c0 + 16]

    def bond_re(r, a, b):
        result(2, r, weight * (0.5 * (a + b)))
        m.put("Yr", r, 0.25 * a + 0.5 * b)

    def bond_im(r, a, b, c, d):
        a, c = a - b, c - d
        result(3, r, weight * (0.5 * (a + c)))
        m.put("Yi", r, 0.25 * a + 0.5 * c)

    def bond():
        pieces(bond_re, m.mm(v, W) + m.mm(u, W, True), m.mm(U, Gs) + m.mm(T, Gd))
        pieces(bond_im, m.mm(u, W), m.mm(v, W, True), m.mm(U, Gd), m.mm(T, Gs))

    def new_w(r, a, b):
        w = m.load(f"w{i}", r) + a - b
        m.store("Wfull", r, w)
        if i:
            m.put(f"W{i}", r, w)

    def density():
        pieces(new_w, m.mm("Yr", v, True) + m.mm("Yi", u, True) + m.mm(u, "Yr", True), m.mm(v, "Yi", True))

    def dens(r, turned):
        a = m.load("Wfull", r)
        result(0, r, weight * (0.5 * (a + turned)))
        result(1, r, weight * (0.5 * (a - turned)))

    def report():
        pieces(dens, m.turned("Wfull"))

    def carry():
        pieces(lambda r, a: m.put("Qr", r, 0.5 * a), m.mm(u, Gd) + m.mm(v, Gs))
        pieces(lambda r, a, b: m.put("Qi", r, 0.5 * (a - b)), m.mm(u, Gs), m.mm(v, Gd))

    def spread():
        pieces(lambda r, a: m.put(f"Gs{i}", r, m.load(f"gs{i}", r) + a), m.mm("Qr", u, True) + m.mm("Qi", v, True))
        pieces(lambda r, a, b: m.put(f"Gd{i}", r, m.load(f"gd{i}", r) + a - b), m.mm("Qr", v, True), m.mm("Qi", u, True))

    return bond, density, report, carry, spread


def forward_kernel(*refs):
    arrays, (keep, send, kept_pairs, kept_full, sides, pairs, full, done), local, sems = refs[4:12], refs[12:20], refs[20:28], refs[28]
    pe, pk, elev, mlev = refs[:4]
    etab, mtab, fermi, kind, broad, kdiag, onsite, coup = local
    small = [pltpu.make_async_copy(arrays[n], local[n], sems.at[n]) for n in range(6)]
    blocks = [pltpu.make_async_copy(arrays[6].at[n], onsite.at[n], sems.at[6 + n]) for n in range(5)]
    hops = pltpu.make_async_copy(arrays[7], coup, sems.at[11])
    for copy in small + blocks[:1] + [hops] + blocks[1:]:
        copy.start()
    m = Parts(pairs, full, kept_pairs, kept_full)
    where = lax.axis_index("layer")
    sides[0] = jnp.full((16, N), (((where ^ (where >> 1)) & 1) == 1).astype(f32))
    sides[1] = jnp.full((16, N), (where >= 2).astype(f32))
    for copy in small:
        copy.wait()
    e = pe[0]
    k = pk[0]
    weight = jnp.full((1, N), etab[elev[0]] * mtab[mlev[0]] * (1.0 / 256), f32)
    kept_full[KEPT_FULL.index("weight"), 0:8, :] = jnp.broadcast_to(weight, (8, N))

    def source(i):
        return broad[i : i + 1, :] * jax.nn.sigmoid(jnp.full((1, N), (fermi[i] - e) / 0.25, f32))

    def real_part(i, r):
        return m.load("mr", r) if i else onsite[0, r, :]

    def own_energy(i):
        def post(r, s, d):
            m.store("mr", r, onsite[i, r, :] + 0.5 * (s + d))
            m.store("mi", r, 0.5 * (s - d))

        blocks[i].wait()
        pieces(post, m.mm(f"Vt{i - 1}", f"u{i - 1}"), m.mm(f"Vt{i - 1}", f"v{i - 1}"))

    def scale(i):
        dr = jnp.zeros((1, N), f32)
        di = jnp.zeros((1, N), f32)
        for c0 in range(0, N, CH):
            r = slice(c0, c0 + CH)
            dr = dr + jnp.sum(jnp.where(eye(r), real_part(i, r), 0.0), axis=0, keepdims=True)
            if i:
                di = di + jnp.sum(jnp.where(eye(r), m.load("mi", r), 0.0), axis=0, keepdims=True)
        dr = e - k * kdiag[i : i + 1, :] - dr
        di = 0.5 * broad[i : i + 1, :] - di
        modulus = dr * dr + di * di
        zr = dr / modulus
        zi = -di / modulus
        size = jnp.sqrt(zr * zr + zi * zi)
        large = jnp.sqrt(0.5 * (size + jnp.abs(zr)))
        other = 0.5 * zi / large
        rr = jnp.where(zr >= 0.0, large, jnp.abs(other))
        ri = jnp.where(zr >= 0.0, other, jnp.where(zi < 0.0, -large, large))

        def post(r):
            mask = eye(r)
            cr = jnp.sum(jnp.where(mask, rr, 0.0), axis=1, keepdims=True)
            ci = jnp.sum(jnp.where(mask, ri, 0.0), axis=1, keepdims=True)
            a = cr * rr - ci * ri
            b = cr * ri + ci * rr
            m.store("or", r, a)
            m.store("oi", r, b)
            er = jnp.where(mask, 0.0, -real_part(i, r))
            if i:
                ei = jnp.where(mask, 0.0, -m.load("mi", r))
                hr, hi = er * a - ei * b, er * b + ei * a
            else:
                hr, hi = er * a, er * b
            m.store("hr", r, hr)
            m.store("hi", r, hi)
            m.put("Hr", r, hr)
            m.put("Hi", r, hi)
            m.put("Hs", r, hr + hi)

        pieces(post)

    def square():
        def post(r, a, b, c):
            m.store("sr", r, a - b)
            m.store("si", r, c - a - b)
            m.put("Sr", r, a - b)
            m.put("Sa", r, c - 2.0 * a)
            m.put("Sb", r, c - 2.0 * b)

        pieces(post, m.mm("Hr", "Hr"), m.mm("Hi", "Hi"), m.mm("Hs", "Hs"))

    def green(i):
        def post(r, k1, k2, k3):
            kr = m.load("sr", r) - m.load("hr", r) - (k1 - k3) + jnp.where(eye(r), 1.0, 0.0)
            ki = m.load("si", r) - m.load("hi", r) - (k1 + k2)
            a = m.load("or", r)
            b = m.load("oi", r)
            gr = kr * a - ki * b
            gi = kr * b + ki * a
            m.put(f"Gs{i}" if i == 4 else f"s{i % 2}", r, gr + gi)
            m.put(f"Gd{i}" if i == 4 else f"d{i % 2}", r, gr - gi)
            if 0 < i < 4:
                m.store(f"gs{i}", r, gr + gi)
                m.store(f"gd{i}", r, gr - gi)
            if i == 0:
                m.put("p0", r, gr * source(0))
                m.put("q0", r, gi * source(0))

        pieces(post, m.mm("Hs", "Sr"), m.mm("Hr", "Sa"), m.mm("Hi", "Sb"))

    def hop(i):
        pieces(lambda r, u, v: (m.put(f"u{i}", r, u), m.put(f"v{i}", r, v)), m.mm(f"s{i % 2}", f"V{i}"), m.mm(f"d{i % 2}", f"V{i}"))

    def names(i):
        return ("Gs4", "Gd4") if i == 4 else (f"s{i % 2}", f"d{i % 2}")

    def inflow(i):
        gamma = source(i)
        pieces(lambda r, y: m.put(f"C{i % 2}", r, y + jnp.where(eye(r), gamma, 0.0)), m.mm(f"Vt{i - 1}", f"U{i - 1}"))

    def dressed_re(i):
        s, d = names(i)
        C = f"C{i % 2}"
        pieces(lambda r, p: m.put(f"p{i % 2}", r, 0.5 * p), m.mm(d, C) + m.mm(s, C, True))

    def dressed_im(i):
        s, d = names(i)
        C = f"C{i % 2}"
        pieces(lambda r, a, b: m.put(f"q{i % 2}", r, 0.5 * (a - b)), m.mm(s, C), m.mm(d, C, True))

    def lesser(i):
        s, d = names(i)

        def post(r, w):
            if i < 4:
                m.store(f"w{i}", r, w)
                m.put("Wl", r, w)
            else:
                m.put("W4", r, w)

        pieces(post, m.mm(f"p{i % 2}", d) + m.mm(f"q{i % 2}", s))

    def lesser_turned(i):
        pieces(lambda r, x: m.put("Wt", r, x), m.turned(f"w{i}"))

    def lesser_hop(i):
        pieces(lambda r, a, b: (m.put(f"U{i}", r, a), m.put(f"T{i}", r, b)), m.mm("Wl", f"V{i}"), m.mm("Wt", f"V{i}"))

    blocks[0].wait()
    scale(0)
    square()
    hops.wait()
    for i in range(4):
        pieces(lambda r, x: m.put(f"V{i}", r, x), coup[kind[i]])
        pieces(lambda r, x: m.put(f"Vt{i}", r, x), coup[kind[i]].T)
    green(0)
    hop(0)
    for i in range(1, 5):
        own_energy(i)
        if i > 1:
            dressed_re(i - 1)
        scale(i)
        if i > 1:
            dressed_im(i - 1)
        square()
        lesser(i - 1)
        lesser_turned(i - 1)
        green(i)
        lesser_hop(i - 1)
        if i < 4:
            hop(i)
        inflow(i)
    steps = {i: back_products(m, i, weight, done) for i in (3, 2, 1)}
    dressed_re(4)
    steps[3][3]()
    dressed_im(4)
    lesser(4)
    steps[3][4]()
    steps[3][0]()
    steps[2][3]()
    steps[3][1]()
    steps[2][4]()
    steps[3][2]()
    hand_out(3, done, keep, send)
    steps[2][0]()
    steps[1][3]()
    steps[2][1]()
    steps[1][4]()
    steps[2][2]()
    hand_out(2, done, keep, send)


def third_kernel(kept_pairs, kept_full, next_pair, keep, send, pairs, full, done):
    m = Parts(pairs, full, kept_pairs, kept_full)
    m.kept["W1"] = (next_pair, 0)
    for step in back_products(m, 1, kept_full[KEPT_FULL.index("weight"), 0:1, :], done)[:3]:
        step()
    hand_out(1, done, keep, send)


def last_kernel(kept_pairs, kept_full, next_pair, keep, send, pairs, full, done):
    m = Parts(pairs, full, kept_pairs, kept_full)
    m.kept["W1"] = (next_pair, 0)
    for step in back_products(m, 0, kept_full[KEPT_FULL.index("weight"), 0:1, :], done)[:3]:
        step()
    hand_out(0, done, keep, send)


def cost(products):
    return pl.CostEstimate(flops=products * 6 * N**3, bytes_accessed=8 * 2**20, transcendentals=0)


BLOCK = (16, 4, 16, N)
HALF_BLOCK = (8, 4, 16, N)


def forward(arrays):
    smem = pl.BlockSpec(memory_space=pltpu.SMEM)
    vmem = pl.BlockSpec(memory_space=pltpu.VMEM)
    hbm = pl.BlockSpec(memory_space=pltpu.HBM)
    return pl.pallas_call(
        forward_kernel,
        out_shape=(
            jax.ShapeDtypeStruct(BLOCK, f32),
            jax.ShapeDtypeStruct(BLOCK, f32),
            jax.ShapeDtypeStruct((len(KEPT), 2, N, N), bf16),
            jax.ShapeDtypeStruct((len(KEPT_FULL), N, N), f32),
            jax.ShapeDtypeStruct((2, 16, N), f32),
        ),
        in_specs=[smem] * 4 + [hbm] * 8,
        out_specs=(vmem,) * 5,
        scratch_shapes=[
            pltpu.VMEM((56, 2, N, N), bf16),
            pltpu.VMEM((18, N, N), f32),
            pltpu.VMEM((4, 16, 16, N), f32),
            pltpu.SMEM((8,), f32),
            pltpu.SMEM((8,), f32),
            pltpu.SMEM((5,), f32),
            pltpu.SMEM((4,), jnp.int32),
            pltpu.VMEM((5, N), f32),
            pltpu.VMEM((5, N), f32),
            pltpu.VMEM((5, N, N), f32),
            pltpu.VMEM((3, N, N), f32),
            pltpu.SemaphoreType.DMA((12,)),
        ],
        compiler_params=pltpu.CompilerParams(vmem_limit_bytes=32 * 1024 * 1024),
        cost_estimate=cost(132),
    )(*arrays[:4], *[pltpu.with_memory_space_constraint(a, pltpu.HBM) for a in arrays[4:]])


def third(kept_pairs, kept_full):
    vmem = pl.BlockSpec(memory_space=pltpu.VMEM)
    return pl.pallas_call(
        third_kernel,
        out_shape=(
            jax.ShapeDtypeStruct((1, 2, N, N), bf16),
            jax.ShapeDtypeStruct(HALF_BLOCK, f32),
            jax.ShapeDtypeStruct(HALF_BLOCK, f32),
        ),
        in_specs=[vmem] * 2,
        out_specs=(vmem,) * 3,
        scratch_shapes=[
            pltpu.VMEM((3, 2, N, N), bf16),
            pltpu.VMEM((1, N, N), f32),
            pltpu.VMEM((4, 16, 16, N), f32),
        ],
        compiler_params=pltpu.CompilerParams(vmem_limit_bytes=12 * 1024 * 1024),
        cost_estimate=cost(12),
    )(kept_pairs, kept_full)


def last(kept_pairs, kept_full, next_pair):
    vmem = pl.BlockSpec(memory_space=pltpu.VMEM)
    return pl.pallas_call(
        last_kernel,
        out_shape=(jax.ShapeDtypeStruct(HALF_BLOCK, f32), jax.ShapeDtypeStruct(HALF_BLOCK, f32)),
        in_specs=[vmem] * 3,
        out_specs=(vmem,) * 2,
        scratch_shapes=[
            pltpu.VMEM((3, 2, N, N), bf16),
            pltpu.VMEM((1, N, N), f32),
            pltpu.VMEM((4, 16, 16, N), f32),
        ],
        compiler_params=pltpu.CompilerParams(vmem_limit_bytes=12 * 1024 * 1024),
        cost_estimate=cost(12),
    )(kept_pairs, kept_full, next_pair)


def swapped(x, axes, partner):
    count = 1
    for a in axes:
        count *= lax.axis_size(a)
    return lax.ppermute(x, axes, [(i, partner(i)) for i in range(count)])


def over_core(x):
    return swapped(x, ("energy",), lambda i: i ^ 1)


def over_x(x, turn):
    return swapped(x, ("energy",), lambda i: i ^ (12 if (i & 1) ^ turn else 4))


def over_y(x, step):
    return swapped(x, ("layer",), lambda i: i ^ step)


def over_rest(x, turn):
    return swapped(x, ("energy", "layer"), lambda i: i ^ (8 if ((i >> 2) & 1) ^ turn else 1))


def over_mixed(x, turn):
    return swapped(x, ("energy",), lambda i: i ^ ((12, 4)[i & 1] if (i & 1) == turn else 2))


def halves(mine, other):
    count = mine.shape[0] // 2
    return mine[:count] + other[:count], mine[count:] + other[count:]


def per_device(energies, momenta, energy_level, momentum_level, energy_table, momentum_table, onsite, broad, kdiag, fermi, couplings, bond_kind):
    keep_high, send_high, kept_pairs, kept_full, sides = forward(
        (energies, momenta, energy_level, momentum_level, energy_table, momentum_table, fermi, bond_kind, broad, kdiag, onsite, couplings)
    )
    got_high = over_core(send_high)
    next_pair, keep_1, send_1 = third(kept_pairs, kept_full)
    high, away_high = halves(keep_high, got_high)
    high, away_high, next_pair, send_1 = lax.optimization_barrier((high, away_high, next_pair, send_1))
    got_high = over_rest(away_high, 0)
    got_1 = over_core(send_1)
    keep_0, send_0 = last(kept_pairs, kept_full, next_pair)
    got_0 = over_core(send_0)
    low_1, low_0 = keep_1, keep_0
    low_1, away_1 = halves(keep_1, got_1)
    got_1 = over_x(away_1, 0)
    low_0, away_0 = halves(keep_0, got_0)
    got_0 = over_x(away_0, 0)
    for step in range(3):
        high, away_high = halves(high, got_high)
        got_high = over_x(away_high, step - 1) if step else over_rest(away_high, 1)
        if step == 2:
            break
        if step:
            low, away = halves(low, got)
        else:
            pairs = [halves(low_1, got_1), halves(low_0, got_0)]
            low, away = (jnp.stack([p[n] for p in pairs], 1) for n in range(2))
        got = over_mixed(away, step)
    high = high[0] + got_high[0]
    low_1, low_0 = (low[0, n] + got[0, n] for n in range(2))
    odd, upper = sides[0] > 0.5, sides[1] > 0.5
    low, low_away = jnp.where(odd, low_1, low_0), jnp.where(odd, low_0, low_1)
    count = lax.axis_size("layer") // 2
    beside = lax.ppermute(low_away, "layer", [(i, i ^ 1) for i in range(count)])
    across = lax.ppermute(low_away, "layer", [(i, i ^ 2) for i in range(count, 2 * count)])
    opposite = over_y(jnp.where(upper, low, high), 3)
    mine = (jnp.where(upper, high, low) + opposite) + (beside + across)
    near, far, both = (swapped(mine, ("kpt",), lambda i, s=s: i ^ s) for s in (1, 2, 3))
    total = (mine + near) + (far + both)
    return total[None, :2], total[None, 2:]


def solution(mesh):
    return jax.shard_map(
        per_device,
        mesh=mesh,
        in_specs=(P(("energy", "layer")), P("kpt"), P(("energy", "layer")), P("kpt"), P(), P(), P(), P(), P(), P(), P(), P()),
        out_specs=(P("layer", None, "energy", None), P("layer", None, "energy", None)),
        check_vma=False,
    )
```

```python
import jax
import jax.numpy as jnp
from jax import lax
from jax.experimental import pallas as pl
from jax.experimental.pallas import tpu as pltpu
from jax.sharding import PartitionSpec as P


N = 256
CH = 32
f32 = jnp.float32
bf16 = jnp.bfloat16
KEPT = ("u0", "v0", "U0", "T0", "u1", "v1", "U1", "T1", "W2", "Gs2", "Gd2", "Gs1", "Gd1")
KEPT_FULL = ("w0", "w1", "weight")


def step_of(at, swap):
    first, second = at >> 1, at & 1
    plain = first ^ (3 * second)
    return plain ^ (swap * 2 * (first ^ second))


class Parts:
    def __init__(self, pairs, full, kept_pairs=None, kept_full=None):
        self.pairs, self.full = pairs, full
        self.at, self.full_at = {}, {}
        self.kept = {} if kept_pairs is None else {n: (kept_pairs, i) for i, n in enumerate(KEPT)}
        self.kept_full = {} if kept_full is None else {n: (kept_full, i) for i, n in enumerate(KEPT_FULL)}

    def pair(self, name):
        if name in self.kept:
            return self.kept[name]
        i = self.at.setdefault(name, len(self.at))
        assert i < self.pairs.shape[0]
        return self.pairs, i

    def whole(self, name):
        if name in self.kept_full:
            return self.kept_full[name]
        i = self.full_at.setdefault(name, len(self.full_at))
        assert i < self.full.shape[0]
        return self.full, i

    def put(self, name, r, x):
        ref, i = self.pair(name)
        high = x.astype(bf16)
        ref[i, 0, r, :] = high
        ref[i, 1, r, :] = (x - high.astype(f32)).astype(bf16)

    def store(self, name, r, x):
        ref, i = self.whole(name)
        ref[i, r, :] = x

    def load(self, name, r):
        ref, i = self.whole(name)
        return ref[i, r, :]

    def turned(self, name):
        ref, i = self.whole(name)
        return ref[i].T

    def mm(self, left, right, turn=False):
        a, i = self.pair(left)
        b, j = self.pair(right)
        contract = (((1,), (1 if turn else 0,)), ((), ()))

        def dot(x, y):
            return lax.dot_general(x, y, contract, preferred_element_type=f32)

        high = a[i, 0]
        return dot(high, b[j, 0]) + dot(high, b[j, 1]) + dot(a[i, 1], b[j, 0])


def pieces(post, *values):
    for c0 in range(0, N, CH):
        r = slice(c0, c0 + CH)
        post(r, *[v[r] for v in values])


def eye(r):
    rows = lax.broadcasted_iota(jnp.int32, (CH, N), 0) + r.start
    return rows == lax.broadcasted_iota(jnp.int32, (CH, N), 1)


def hand_out(layer, parts, keep, send):
    energy = lax.axis_index("energy")
    core = energy & 1
    my_x, my_z = energy >> 2, (energy >> 1) & 1
    where_y = lax.axis_index("layer")
    y_at = (layer ^ (layer >> 1) ^ where_y ^ (where_y >> 1)) & 1
    for core_at, to in ((0, keep), (1, send)):
        turn = core ^ core_at
        for x_at in range(4):
            x_from = my_x ^ step_of(x_at, turn)
            for z_at in range(2):
                chunk = x_from * 4 + (my_z ^ z_at) * 2 + turn
                if layer >= 2:
                    spot = (y_at * (2 - turn) + z_at * (1 + turn)) * 4 + x_at
                else:
                    spot = (x_at >> 1) * 4 + (x_at & 1) * (2 - turn) + z_at * (1 + turn)
                for comp in range(4):
                    ref, n = parts[comp]
                    to[spot, comp] = ref[n, chunk]


def back_products(m, i, weight, parts):
    u, v, U, T = f"u{i}", f"v{i}", f"U{i}", f"T{i}"
    W, Gs, Gd = f"W{i + 1}", f"Gs{i + 1}", f"Gd{i + 1}"

    def result(comp, r, x):
        ref, n = parts[comp]
        for c0 in range(0, CH, 16):
            ref[n, (r.start + c0) // 16] = x[c0 : c0 + 16]

    def bond_re(r, a, b):
        result(2, r, weight * (0.5 * (a + b)))
        m.put("Yr", r, 0.25 * a + 0.5 * b)

    def bond_im(r, a, b, c, d):
        a, c = a - b, c - d
        result(3, r, weight * (0.5 * (a + c)))
        m.put("Yi", r, 0.25 * a + 0.5 * c)

    def bond():
        pieces(bond_re, m.mm(v, W) + m.mm(u, W, True), m.mm(U, Gs) + m.mm(T, Gd))
        pieces(bond_im, m.mm(u, W), m.mm(v, W, True), m.mm(U, Gd), m.mm(T, Gs))

    def new_w(r, a, b):
        w = m.load(f"w{i}", r) + a - b
        m.store("Wfull", r, w)
        if i:
            m.put(f"W{i}", r, w)

    def density():
        pieces(new_w, m.mm("Yr", v, True) + m.mm("Yi", u, True) + m.mm(u, "Yr", True), m.mm(v, "Yi", True))

    def dens(r, turned):
        a = m.load("Wfull", r)
        result(0, r, weight * (0.5 * (a + turned)))
        result(1, r, weight * (0.5 * (a - turned)))

    def report():
        pieces(dens, m.turned("Wfull"))

    def carry():
        pieces(lambda r, a: m.put("Qr", r, 0.5 * a), m.mm(u, Gd) + m.mm(v, Gs))
        pieces(lambda r, a, b: m.put("Qi", r, 0.5 * (a - b)), m.mm(u, Gs), m.mm(v, Gd))

    def spread():
        pieces(lambda r, a: m.put(f"Gs{i}", r, m.load(f"gs{i}", r) + a), m.mm("Qr", u, True) + m.mm("Qi", v, True))
        pieces(lambda r, a, b: m.put(f"Gd{i}", r, m.load(f"gd{i}", r) + a - b), m.mm("Qr", v, True), m.mm("Qi", u, True))

    return bond, density, report, carry, spread


def forward_kernel(*refs):
    arrays, (keep, send, kept_pairs, kept_full, sides, pairs, full, done), local, sems = refs[4:12], refs[12:20], refs[20:28], refs[28]
    pe, pk, elev, mlev = refs[:4]
    etab, mtab, fermi, kind, broad, kdiag, onsite, coup = local
    small = [pltpu.make_async_copy(arrays[n], local[n], sems.at[n]) for n in range(6)]
    blocks = [pltpu.make_async_copy(arrays[6].at[n], onsite.at[n], sems.at[6 + n]) for n in range(5)]
    hops = pltpu.make_async_copy(arrays[7], coup, sems.at[11])
    for copy in small + blocks[:1] + [hops] + blocks[1:]:
        copy.start()
    m = Parts(pairs, full, kept_pairs, kept_full)
    where = lax.axis_index("layer")
    sides[0] = jnp.full((16, N), (((where ^ (where >> 1)) & 1) == 1).astype(f32))
    sides[1] = jnp.full((16, N), (where >= 2).astype(f32))
    for copy in small:
        copy.wait()
    e = pe[0]
    k = pk[0]
    weight = jnp.full((1, N), etab[elev[0]] * mtab[mlev[0]] * (1.0 / 256), f32)
    kept_full[KEPT_FULL.index("weight"), 0:8, :] = jnp.broadcast_to(weight, (8, N))

    def source(i):
        return broad[i : i + 1, :] * jax.nn.sigmoid(jnp.full((1, N), (fermi[i] - e) / 0.25, f32))

    def real_part(i, r):
        return m.load("mr", r) if i else onsite[0, r, :]

    def own_energy(i):
        def post(r, s, d):
            m.store("mr", r, onsite[i, r, :] + 0.5 * (s + d))
            m.store("mi", r, 0.5 * (s - d))

        blocks[i].wait()
        pieces(post, m.mm(f"Vt{i - 1}", f"u{i - 1}"), m.mm(f"Vt{i - 1}", f"v{i - 1}"))

    def scale(i):
        dr = jnp.zeros((1, N), f32)
        di = jnp.zeros((1, N), f32)
        for c0 in range(0, N, CH):
            r = slice(c0, c0 + CH)
            dr = dr + jnp.sum(jnp.where(eye(r), real_part(i, r), 0.0), axis=0, keepdims=True)
            if i:
                di = di + jnp.sum(jnp.where(eye(r), m.load("mi", r), 0.0), axis=0, keepdims=True)
        dr = e - k * kdiag[i : i + 1, :] - dr
        di = 0.5 * broad[i : i + 1, :] - di
        modulus = dr * dr + di * di
        zr = dr / modulus
        zi = -di / modulus
        size = jnp.sqrt(zr * zr + zi * zi)
        large = jnp.sqrt(0.5 * (size + jnp.abs(zr)))
        other = 0.5 * zi / large
        rr = jnp.where(zr >= 0.0, large, jnp.abs(other))
        ri = jnp.where(zr >= 0.0, other, jnp.where(zi < 0.0, -large, large))

        def post(r):
            mask = eye(r)
            cr = jnp.sum(jnp.where(mask, rr, 0.0), axis=1, keepdims=True)
            ci = jnp.sum(jnp.where(mask, ri, 0.0), axis=1, keepdims=True)
            a = cr * rr - ci * ri
            b = cr * ri + ci * rr
            m.store("or", r, a)
            m.store("oi", r, b)
            er = jnp.where(mask, 0.0, -real_part(i, r))
            if i:
                ei = jnp.where(mask, 0.0, -m.load("mi", r))
                hr, hi = er * a - ei * b, er * b + ei * a
            else:
                hr, hi = er * a, er * b
            m.store("hr", r, hr)
            m.store("hi", r, hi)
            m.put("Hr", r, hr)
            m.put("Hi", r, hi)
            m.put("Hs", r, hr + hi)

        pieces(post)

    def square():
        def post(r, a, b, c):
            m.store("sr", r, a - b)
            m.store("si", r, c - a - b)
            m.put("Sr", r, a - b)
            m.put("Sa", r, c - 2.0 * a)
            m.put("Sb", r, c - 2.0 * b)

        pieces(post, m.mm("Hr", "Hr"), m.mm("Hi", "Hi"), m.mm("Hs", "Hs"))

    def green(i):
        def post(r, k1, k2, k3):
            kr = m.load("sr", r) - m.load("hr", r) - (k1 - k3) + jnp.where(eye(r), 1.0, 0.0)
            ki = m.load("si", r) - m.load("hi", r) - (k1 + k2)
            a = m.load("or", r)
            b = m.load("oi", r)
            gr = kr * a - ki * b
            gi = kr * b + ki * a
            m.put(f"Gs{i}" if i == 4 else f"s{i % 2}", r, gr + gi)
            m.put(f"Gd{i}" if i == 4 else f"d{i % 2}", r, gr - gi)
            if 0 < i < 4:
                m.store(f"gs{i}", r, gr + gi)
                m.store(f"gd{i}", r, gr - gi)
            if i == 0:
                m.put("p0", r, gr * source(0))
                m.put("q0", r, gi * source(0))

        pieces(post, m.mm("Hs", "Sr"), m.mm("Hr", "Sa"), m.mm("Hi", "Sb"))

    def hop(i):
        pieces(lambda r, u, v: (m.put(f"u{i}", r, u), m.put(f"v{i}", r, v)), m.mm(f"s{i % 2}", f"V{i}"), m.mm(f"d{i % 2}", f"V{i}"))

    def names(i):
        return ("Gs4", "Gd4") if i == 4 else (f"s{i % 2}", f"d{i % 2}")

    def inflow(i):
        gamma = source(i)
        pieces(lambda r, y: m.put(f"C{i % 2}", r, y + jnp.where(eye(r), gamma, 0.0)), m.mm(f"Vt{i - 1}", f"U{i - 1}"))

    def dressed_re(i):
        s, d = names(i)
        C = f"C{i % 2}"
        pieces(lambda r, p: m.put(f"p{i % 2}", r, 0.5 * p), m.mm(d, C) + m.mm(s, C, True))

    def dressed_im(i):
        s, d = names(i)
        C = f"C{i % 2}"
        pieces(lambda r, a, b: m.put(f"q{i % 2}", r, 0.5 * (a - b)), m.mm(s, C), m.mm(d, C, True))

    def lesser(i):
        s, d = names(i)

        def post(r, w):
            if i < 4:
                m.store(f"w{i}", r, w)
                m.put("Wl", r, w)
            else:
                m.put("W4", r, w)

        pieces(post, m.mm(f"p{i % 2}", d) + m.mm(f"q{i % 2}", s))

    def lesser_turned(i):
        pieces(lambda r, x: m.put("Wt", r, x), m.turned(f"w{i}"))

    def lesser_hop(i):
        pieces(lambda r, a, b: (m.put(f"U{i}", r, a), m.put(f"T{i}", r, b)), m.mm("Wl", f"V{i}"), m.mm("Wt", f"V{i}"))

    blocks[0].wait()
    scale(0)
    square()
    hops.wait()
    for i in range(4):
        pieces(lambda r, x: m.put(f"V{i}", r, x), coup[kind[i]])
        pieces(lambda r, x: m.put(f"Vt{i}", r, x), coup[kind[i]].T)
    green(0)
    hop(0)
    for i in range(1, 5):
        own_energy(i)
        if i > 1:
            dressed_re(i - 1)
        scale(i)
        if i > 1:
            dressed_im(i - 1)
        square()
        lesser(i - 1)
        lesser_turned(i - 1)
        green(i)
        lesser_hop(i - 1)
        if i < 4:
            hop(i)
        inflow(i)
    steps = {i: back_products(m, i, weight, [(done, n) for n in range(4)]) for i in (3, 2, 1)}
    dressed_re(4)
    steps[3][3]()
    dressed_im(4)
    lesser(4)
    steps[3][4]()
    steps[3][0]()
    steps[2][3]()
    steps[3][1]()
    steps[2][4]()
    steps[3][2]()
    hand_out(3, [(done, n) for n in range(4)], keep, send)
    steps[2][0]()
    steps[1][3]()
    steps[2][1]()
    steps[1][4]()
    steps[2][2]()
    hand_out(2, [(done, n) for n in range(4)], keep, send)


def third_kernel(kept_pairs, kept_full, next_pair, keep, send, pairs, full, done):
    m = Parts(pairs, full, kept_pairs, kept_full)
    m.kept["W1"] = (next_pair, 0)
    for step in back_products(m, 1, kept_full[KEPT_FULL.index("weight"), 0:1, :], [(done, n) for n in range(4)])[:3]:
        step()
    hand_out(1, [(done, n) for n in range(4)], keep, send)


def bond_kernel(kept_pairs, kept_full, next_pair, side_pairs, bonds, pairs, full):
    m = Parts(pairs, full, kept_pairs, kept_full)
    m.kept["W1"] = (next_pair, 0)
    m.kept["Yr"] = (side_pairs, 0)
    m.kept["Yi"] = (side_pairs, 1)
    back_products(m, 0, kept_full[KEPT_FULL.index("weight"), 0:1, :], {2: (bonds, 0), 3: (bonds, 1)})[0]()


def density_kernel(kept_pairs, kept_full, side_pairs, bonds, keep, send, pairs, full, done):
    m = Parts(pairs, full, kept_pairs, kept_full)
    m.kept["Yr"] = (side_pairs, 0)
    m.kept["Yi"] = (side_pairs, 1)
    parts = [(done, 0), (done, 1), (bonds, 0), (bonds, 1)]
    for step in back_products(m, 0, kept_full[KEPT_FULL.index("weight"), 0:1, :], parts)[1:3]:
        step()
    hand_out(0, parts, keep, send)


def cost(products):
    return pl.CostEstimate(flops=products * 6 * N**3, bytes_accessed=8 * 2**20, transcendentals=0)


BLOCK = (16, 4, 16, N)
HALF_BLOCK = (8, 4, 16, N)


def forward(arrays):
    smem = pl.BlockSpec(memory_space=pltpu.SMEM)
    vmem = pl.BlockSpec(memory_space=pltpu.VMEM)
    hbm = pl.BlockSpec(memory_space=pltpu.HBM)
    return pl.pallas_call(
        forward_kernel,
        out_shape=(
            jax.ShapeDtypeStruct(BLOCK, f32),
            jax.ShapeDtypeStruct(BLOCK, f32),
            jax.ShapeDtypeStruct((len(KEPT), 2, N, N), bf16),
            jax.ShapeDtypeStruct((len(KEPT_FULL), N, N), f32),
            jax.ShapeDtypeStruct((2, 16, N), f32),
        ),
        in_specs=[smem] * 4 + [hbm] * 8,
        out_specs=(vmem,) * 5,
        scratch_shapes=[
            pltpu.VMEM((56, 2, N, N), bf16),
            pltpu.VMEM((18, N, N), f32),
            pltpu.VMEM((4, 16, 16, N), f32),
            pltpu.SMEM((8,), f32),
            pltpu.SMEM((8,), f32),
            pltpu.SMEM((5,), f32),
            pltpu.SMEM((4,), jnp.int32),
            pltpu.VMEM((5, N), f32),
            pltpu.VMEM((5, N), f32),
            pltpu.VMEM((5, N, N), f32),
            pltpu.VMEM((3, N, N), f32),
            pltpu.SemaphoreType.DMA((12,)),
        ],
        compiler_params=pltpu.CompilerParams(vmem_limit_bytes=32 * 1024 * 1024),
        cost_estimate=cost(132),
    )(*arrays[:4], *[pltpu.with_memory_space_constraint(a, pltpu.HBM) for a in arrays[4:]])


def third(kept_pairs, kept_full):
    vmem = pl.BlockSpec(memory_space=pltpu.VMEM)
    return pl.pallas_call(
        third_kernel,
        out_shape=(
            jax.ShapeDtypeStruct((1, 2, N, N), bf16),
            jax.ShapeDtypeStruct(HALF_BLOCK, f32),
            jax.ShapeDtypeStruct(HALF_BLOCK, f32),
        ),
        in_specs=[vmem] * 2,
        out_specs=(vmem,) * 3,
        scratch_shapes=[
            pltpu.VMEM((3, 2, N, N), bf16),
            pltpu.VMEM((1, N, N), f32),
            pltpu.VMEM((4, 16, 16, N), f32),
        ],
        compiler_params=pltpu.CompilerParams(vmem_limit_bytes=12 * 1024 * 1024),
        cost_estimate=cost(12),
    )(kept_pairs, kept_full)


def bond(kept_pairs, kept_full, next_pair):
    vmem = pl.BlockSpec(memory_space=pltpu.VMEM)
    return pl.pallas_call(
        bond_kernel,
        out_shape=(jax.ShapeDtypeStruct((2, 2, N, N), bf16), jax.ShapeDtypeStruct((2, 16, 16, N), f32)),
        in_specs=[vmem] * 3,
        out_specs=(vmem,) * 2,
        scratch_shapes=[pltpu.VMEM((1, 2, N, N), bf16), pltpu.VMEM((1, N, N), f32)],
        compiler_params=pltpu.CompilerParams(vmem_limit_bytes=12 * 1024 * 1024),
        cost_estimate=cost(8),
    )(kept_pairs, kept_full, next_pair)


def density(kept_pairs, kept_full, side_pairs, bonds):
    vmem = pl.BlockSpec(memory_space=pltpu.VMEM)
    return pl.pallas_call(
        density_kernel,
        out_shape=(jax.ShapeDtypeStruct(HALF_BLOCK, f32), jax.ShapeDtypeStruct(HALF_BLOCK, f32)),
        in_specs=[vmem] * 4,
        out_specs=(vmem,) * 2,
        scratch_shapes=[
            pltpu.VMEM((1, 2, N, N), bf16),
            pltpu.VMEM((1, N, N), f32),
            pltpu.VMEM((2, 16, 16, N), f32),
        ],
        compiler_params=pltpu.CompilerParams(vmem_limit_bytes=12 * 1024 * 1024),
        cost_estimate=cost(4),
    )(kept_pairs, kept_full, side_pairs, bonds)


def swapped(x, axes, partner):
    count = 1
    for a in axes:
        count *= lax.axis_size(a)
    return lax.ppermute(x, axes, [(i, partner(i)) for i in range(count)])


def over_core(x):
    return swapped(x, ("energy",), lambda i: i ^ 1)


def over_x(x, turn):
    return swapped(x, ("energy",), lambda i: i ^ (12 if (i & 1) ^ turn else 4))


def over_y(x, step):
    return swapped(x, ("layer",), lambda i: i ^ step)


def over_rest(x, turn):
    return swapped(x, ("energy", "layer"), lambda i: i ^ (8 if ((i >> 2) & 1) ^ turn else 1))


def over_mixed(x, turn):
    return swapped(x, ("energy",), lambda i: i ^ ((12, 4)[i & 1] if (i & 1) == turn else 2))


def halves(mine, other):
    count = mine.shape[0] // 2
    return mine[:count] + other[:count], mine[count:] + other[count:]


def per_device(energies, momenta, energy_level, momentum_level, energy_table, momentum_table, onsite, broad, kdiag, fermi, couplings, bond_kind):
    keep_high, send_high, kept_pairs, kept_full, sides = forward(
        (energies, momenta, energy_level, momentum_level, energy_table, momentum_table, fermi, bond_kind, broad, kdiag, onsite, couplings)
    )
    got_high = over_core(send_high)
    next_pair, keep_1, send_1 = third(kept_pairs, kept_full)
    high, away_high = halves(keep_high, got_high)
    high, away_high, next_pair, send_1 = lax.optimization_barrier((high, away_high, next_pair, send_1))
    got_high = over_rest(away_high, 0)
    got_1 = over_core(send_1)
    side_pairs, bonds = bond(kept_pairs, kept_full, next_pair)
    low_1, away_1 = halves(keep_1, got_1)
    got_1 = over_x(away_1, 0)
    keep_0, send_0 = density(kept_pairs, kept_full, side_pairs, bonds)
    got_0 = over_core(send_0)
    low_0, away_0 = halves(keep_0, got_0)
    got_0 = over_x(away_0, 0)
    for step in range(3):
        high, away_high = halves(high, got_high)
        got_high = over_x(away_high, step - 1) if step else over_rest(away_high, 1)
        if step == 2:
            break
        low_1, away_1 = halves(low_1, got_1)
        got_1 = over_mixed(away_1, step)
        low_0, away_0 = halves(low_0, got_0)
        got_0 = over_mixed(away_0, step)
    high = high[0] + got_high[0]
    low_1 = low_1[0] + got_1[0]
    low_0 = low_0[0] + got_0[0]
    odd, upper = sides[0] > 0.5, sides[1] > 0.5
    low = jnp.where(odd, low_1, low_0) + over_y(jnp.where(odd, low_0, low_1), 1)
    got = over_y(jnp.where(upper, low, high), 3)
    mine = jnp.where(upper, high, low) + got
    far = swapped(mine, ("kpt",), lambda i: i ^ 2)
    near = swapped(mine, ("kpt",), lambda i: i ^ 1)
    both = swapped(mine, ("kpt",), lambda i: i ^ 3)
    total = (mine + near) + (far + both)
    return total[None, :2], total[None, 2:]


def solution(mesh):
    return jax.shard_map(
        per_device,
        mesh=mesh,
        in_specs=(P(("energy", "layer")), P("kpt"), P(("energy", "layer")), P("kpt"), P(), P(), P(), P(), P(), P(), P(), P()),
        out_specs=(P("layer", None, "energy", None), P("layer", None, "energy", None)),
        check_vma=False,
    )
```
